32 devices in a mesh: dp: 4 (over y, core), tensor: 8 (over z, x).
Axes of the slice: x: 2, y: 2, z: 4, core: 2. Of those that a mesh axis runs over, the one named last changes fastest.
Arguments:
- query_latent: bfloat16 [64, 1536], P(('dp', 'tensor')), may hold values from -40 to 40
- key_value_latent: bfloat16 [64, 512], P(('dp', 'tensor')), may hold values from -40 to 40
- query_gain: float32 [1536], replicated, may hold values from 0.5 to 1.5
- key_value_gain: float32 [512], replicated, may hold values from 0.5 to 1.5
- q_up: bfloat16 [1536, 3072], P(None, 'tensor'), may hold values from -0.625 to 0.625
- kv_up: bfloat16 [512, 4096], P(None, 'tensor'), may hold values from -1 to 1
- grad_q: bfloat16 [64, 3072], P('dp', 'tensor'), may hold values from -0.23925781 to 0.23925781
- grad_kv: bfloat16 [64, 4096], P('dp', 'tensor'), may hold values from -0.23925781 to 0.23925781
Outputs:
- query_latent_gradient: float32 [64, 1536], P(('dp', 'tensor'))
- key_value_latent_gradient: float32 [64, 512], P(('dp', 'tensor'))
- d_q_up: float32 [1536, 3072], P('dp', 'tensor')
- d_kv_up: float32 [512, 4096], P('dp', 'tensor')
The draws below stay inside these ranges and needn't reach their ends.
All inputs are finite; a program needn't handle non-finite values.
Results may differ from the reference program's by a relative error of at most 0.0029.
Values may be sent and summed in bfloat16 or wider, within the bound.
A program may use at most 64 MiB of HBM per device.

```python
import math
import jax
import jax.numpy as jnp
from jax import lax

QL = 1536
KVL = 512
NOPE = 128
ROPE = 64
VDIM = 128
HEADS = 16
TOK_ALL = 64
N_DP = 4


def scaled_latent(key, rows, cols):
    key_rows, key_cols, key_base = jax.random.split(key, 3)
    row_scale = 0.3 * jnp.exp(jax.random.uniform(key_rows, (rows, 1), minval=0.0, maxval=math.log(10.0)))
    col_scale = 0.3 * jnp.exp(jax.random.uniform(key_cols, (1, cols), minval=0.0, maxval=math.log(10.0)))
    base = jax.random.normal(key_base, (rows, cols))
    input_values = jnp.clip(base * row_scale * col_scale, -40.0, 40.0)
    return input_values.astype(jnp.bfloat16)


def draw_query_latent(key, part):
    return scaled_latent(jax.random.fold_in(key, 11), TOK_ALL, QL)


def draw_key_value_latent(key, part):
    return scaled_latent(jax.random.fold_in(key, 23), TOK_ALL, KVL)


def steps_of(own_key, extent, cuts, low, high):
    def one(dim, shards_of):
        heights = jax.random.uniform(jax.random.fold_in(jax.random.fold_in(own_key, 6), dim), (shards_of,), jnp.float32, low / len(cuts), high / len(cuts))
        return jnp.repeat(jnp.exp(heights), extent[dim] // shards_of).reshape((-1,) + (1,) * (len(extent) - dim - 1))

    factor_of = one(*cuts[0])
    for cut in cuts[1:]:
        factor_of = factor_of * one(*cut)
    return factor_of


def centred(key, shape, scale, bound, cuts=(), held_as=jnp.bfloat16):
    drawn = jax.random.normal(key, shape, jnp.float32) * scale
    if len(cuts) > 0:
        drawn = steps_of(key, shape, cuts, -0.22, 0.18) * drawn
    return jnp.clip(drawn, min=-bound, max=bound).astype(held_as)


def setup_inputs(seed: int = 0) -> dict:
    streams_of = jax.random.split(jax.random.key(seed), 9)
    query_latent = draw_query_latent(jax.random.fold_in(streams_of[8], 71), 0)
    key_value_latent = draw_key_value_latent(jax.random.fold_in(streams_of[8], 71), 0)
    query_gain = jnp.clip(1.0 + 0.1 * jax.random.normal(streams_of[2], (QL,), jnp.float32), 0.5, 1.5)
    key_value_gain = jnp.clip(1.0 + 0.1 * jax.random.normal(streams_of[3], (KVL,), jnp.float32), 0.5, 1.5)
    q_up = centred(streams_of[4], (QL, HEADS * (NOPE + ROPE)), (QL // 16) ** -0.5, 0.625, ((1, 8),))
    kv_up = centred(streams_of[5], (KVL, HEADS * (NOPE + VDIM)), (KVL // 16) ** -0.5, 1.0, ((1, 8),))
    grad_q = centred(streams_of[6], (TOK_ALL, HEADS * (NOPE + ROPE)), 0.04, 0.23925781, ((0, 4), (1, 8)))
    grad_kv = centred(streams_of[7], (TOK_ALL, HEADS * (NOPE + VDIM)), 0.04, 0.23925781, ((0, 4), (1, 8)))
    return {"query_latent": query_latent, "key_value_latent": key_value_latent, "query_gain": query_gain, "key_value_gain": key_value_gain, "q_up": q_up, "kv_up": kv_up, "grad_q": grad_q, "grad_kv": grad_kv}


EPS = 1e-06

def apply_norm(raw, norm_gain):
    input_values = raw.astype(jnp.float32)
    inverse_norm = lax.rsqrt(lax.optimization_barrier(jnp.mean(input_values * input_values, axis=-1, keepdims=True)) + EPS)
    unit_input = input_values * inverse_norm
    return (unit_input, inverse_norm, (norm_gain * unit_input).astype(jnp.bfloat16))

def backward_of_norm(incoming_gradient, unit_input, inverse_norm, norm_gain):
    scaled_gradient = norm_gain * incoming_gradient
    mean_correction = lax.optimization_barrier(jnp.mean(scaled_gradient * unit_input, axis=-1, keepdims=True))
    return inverse_norm * (scaled_gradient - unit_input * mean_correction)

def group_weights(normed, cotangent):
    groups = normed.reshape(N_DP, -1, normed.shape[1])
    cot_groups = cotangent.reshape(N_DP, -1, cotangent.shape[1])

    def step(total, pair):
        part = lax.dot_general(pair[0], pair[1], (((0,), (0,)), ((), ())), preferred_element_type=jnp.float32)
        return (total + part, None)
    start = jnp.zeros((normed.shape[1], cotangent.shape[1]), jnp.float32)
    total, unused_item = lax.scan(step, start, (groups, cot_groups))
    return total

def reference(query_latent, key_value_latent, query_gain, key_value_gain, q_up, kv_up, grad_q, grad_kv):
    query_unit, query_inverse_norm, query_normed = apply_norm(query_latent, query_gain)
    key_value_unit, key_value_inverse_norm, key_value_normed = apply_norm(key_value_latent, key_value_gain)
    d_q_up = group_weights(query_normed, grad_q)
    d_kv_up = group_weights(key_value_normed, grad_kv)
    query_norm_gain = lax.dot_general(grad_q, q_up, (((1,), (1,)), ((), ())), preferred_element_type=jnp.float32)
    key_value_norm_gain = lax.dot_general(grad_kv, kv_up, (((1,), (1,)), ((), ())), preferred_element_type=jnp.float32)
    query_latent_gradient = backward_of_norm(query_norm_gain, query_unit, query_inverse_norm, query_gain)
    key_value_latent_gradient = backward_of_norm(key_value_norm_gain, key_value_unit, key_value_inverse_norm, key_value_gain)
    return (query_latent_gradient, key_value_latent_gradient, d_q_up, d_kv_up)
```

```python
import functools

import jax
import jax.numpy as jnp
from jax import lax
from jax.experimental import pallas as pl
from jax.experimental.pallas import tpu as pltpu
from jax.sharding import PartitionSpec as P

EPS = 1e-06
UNROLL = 64
LIMIT = 24 * 1024 * 1024


def repeat(count, step):
    if count <= UNROLL:
        for index in range(count):
            step(index)
    else:

        def body(index, carry):
            step(index)
            return carry

        lax.fori_loop(0, count, body, 0)


def unit_rows(raw):
    values = raw.astype(jnp.float32)
    inverse = lax.rsqrt(jnp.mean(values * values, axis=-1, keepdims=True) + EPS)
    return values * inverse, inverse


def backward_of_norm(incoming, unit, inverse, gain):
    scaled = gain * incoming
    return inverse * (scaled - unit * jnp.mean(scaled * unit, axis=-1, keepdims=True))


def wait_bytes(ref, sem):
    pltpu.make_async_copy(ref, ref, sem).wait()


def exchange(
    n_dp, n_t,
    lq_hbm, lkv_hbm, gain_q_hbm, gain_kv_hbm, q_up_hbm, kv_up_hbm, gq_hbm, gkv_hbm,
    g_recv, all_gq, all_gkv, normed_recv, lq, lkv, gain_q, gain_kv,
    q_up, kv_up, normed_send, g_send,
    load_sem, send_sem, recv_sem,
):
    me_d, me_t = lax.axis_index("dp"), lax.axis_index("tensor")
    me = me_d * n_t + me_t
    devices = n_dp * n_t
    rows = lq.shape[0]
    q_width, kv_width = lq.shape[1], lkv.shape[1]
    q_part, kv_part = q_width // n_dp, kv_width // n_dp

    gq, gkv = all_gq.at[me_d], all_gkv.at[me_d]
    barrier = pltpu.get_barrier_semaphore()

    def far(index):
        step = (index + 1) // 2
        return lax.rem(me_t + n_t // 2 + step * (2 * (index % 2) - 1) + n_t, n_t)

    def peer(offset):
        return lax.rem(me_d + offset % n_dp + 1, n_dp), far(offset // n_dp)

    def greet(index):
        pl.semaphore_signal(
            barrier, inc=1, device_id=peer(index), device_id_type=pl.DeviceIdType.MESH
        )

    repeat(devices - 1, greet)

    pairs = (
        (lq_hbm, lq),
        (lkv_hbm, lkv),
        (gain_q_hbm, gain_q),
        (gain_kv_hbm, gain_kv),
        (gq_hbm, gq),
        (gkv_hbm, gkv),
        (q_up_hbm, q_up),
        (kv_up_hbm, kv_up),
    )
    loads = [
        pltpu.make_async_copy(source, target, load_sem.at[index])
        for index, (source, target) in enumerate(pairs)
    ]
    for load in loads:
        load.start()

    for load in loads[:4]:
        load.wait()
    normed_q = gain_q[...] * unit_rows(lq[...])[0]
    normed_kv = gain_kv[...] * unit_rows(lkv[...])[0]
    for d in range(n_dp):
        piece = jnp.concatenate(
            (
                normed_q[:, d * q_part : (d + 1) * q_part],
                normed_kv[:, d * kv_part : (d + 1) * kv_part],
            ),
            axis=1,
        )
        normed_send[d] = piece.astype(jnp.bfloat16)

    normed_recv[me] = normed_send[me_d]
    pl.semaphore_wait(barrier, devices - 1)

    def send(source, target, kind, device):
        pltpu.make_async_remote_copy(
            src_ref=source,
            dst_ref=target,
            send_sem=send_sem.at[kind],
            recv_sem=recv_sem.at[kind],
            device_id=device,
            device_id_type=pl.DeviceIdType.MESH,
        ).start()

    def send_sums(index):
        t = far(index)
        send(g_send.at[t], g_recv.at[me_t], 0, (me_d, t))

    def send_normed(index):
        d, t = peer(index)
        send(normed_send.at[d], normed_recv.at[me], 1, (d, t))

    def send_grads(index):
        d = lax.rem(me_d + index + 1, n_dp)
        send(gq, all_gq.at[me_d], 2, (d, me_t))
        send(gkv, all_gkv.at[me_d], 3, (d, me_t))

    repeat(devices - 1, send_normed)
    for load in loads[4:6]:
        load.wait()
    repeat(n_dp - 1, send_grads)

    for load in loads[6:]:
        load.wait()
    nt = (((1,), (1,)), ((), ()))
    g_q = lax.dot_general(gq[...], q_up[...], nt, preferred_element_type=jnp.float32)
    g_kv = lax.dot_general(gkv[...], kv_up[...], nt, preferred_element_type=jnp.float32)
    for t in range(n_t):
        g_send[t, :, :q_width] = g_q[t * rows : (t + 1) * rows].astype(g_send.dtype)
        g_send[t, :, q_width:] = g_kv[t * rows : (t + 1) * rows].astype(g_send.dtype)

    repeat(n_t - 1, send_sums)
    g_recv[me_t] = g_send[me_t]
    for sem in (send_sem, recv_sem):
        wait_bytes(g_recv.at[pl.ds(0, n_t - 1)], sem.at[0])
        wait_bytes(all_gq.at[pl.ds(0, n_dp - 1)], sem.at[2])
        wait_bytes(all_gkv.at[pl.ds(0, n_dp - 1)], sem.at[3])
        wait_bytes(normed_recv.at[pl.ds(0, devices - 1)], sem.at[1])


def finish(
    g, gq, gkv, normed_in, lq, lkv, gain_q, gain_kv,
    out_q_hbm, out_kv_hbm, d_q_hbm, d_kv_hbm,
    normed_all, out_q, out_kv, d_q, d_kv,
    store_sem,
):
    stores = [
        pltpu.make_async_copy(source, target, store_sem.at[index])
        for index, (source, target) in enumerate(
            ((d_q, d_q_hbm), (d_kv, d_kv_hbm), (out_q, out_q_hbm), (out_kv, out_kv_hbm))
        )
    ]
    n_t, rows = g.shape[:2]
    devices = normed_in.shape[0]
    q_width = lq.shape[1]
    q_part = d_q.shape[0]
    group = max(1, 8 // rows)

    def gather_rows(index):
        block = jnp.concatenate(
            [normed_in[index * group + k].astype(jnp.float32) for k in range(group)], axis=0
        )
        start = index * group * rows
        if not isinstance(start, int):
            start = pl.multiple_of(start, group * rows)
        normed_all[pl.ds(start, group * rows), :] = block

    repeat(devices // group, gather_rows)
    normed = normed_all[...].astype(jnp.bfloat16)
    tn = (((0,), (0,)), ((), ()))
    tokens = normed.shape[0]
    d_q[...] = lax.dot_general(
        normed[:, :q_part], gq[...].reshape(tokens, -1), tn, preferred_element_type=jnp.float32
    )
    stores[0].start()
    d_kv[...] = lax.dot_general(
        normed[:, q_part:], gkv[...].reshape(tokens, -1), tn, preferred_element_type=jnp.float32
    )
    stores[1].start()
    total = g[0].astype(jnp.float32)
    for t in range(1, n_t):
        total += g[t].astype(jnp.float32)
    out_q[...] = backward_of_norm(total[:, :q_width], *unit_rows(lq[...]), gain_q[...])
    stores[2].start()
    out_kv[...] = backward_of_norm(total[:, q_width:], *unit_rows(lkv[...]), gain_kv[...])
    stores[3].start()
    for store in stores:
        store.wait()


def solution(mesh):
    n_dp, n_t = mesh.shape["dp"], mesh.shape["tensor"]

    def body(latent_q, latent_kv, gain_q, gain_kv, q_up, kv_up, grad_q, grad_kv):
        rows, q_width = latent_q.shape
        kv_width = latent_kv.shape[1]
        q_part, kv_part = q_width // n_dp, kv_width // n_dp
        part = q_part + kv_part
        width = q_width + kv_width
        devices = n_dp * n_t
        f32, bf16 = jnp.float32, jnp.bfloat16
        operands = (latent_q, latent_kv, gain_q, gain_kv, q_up, kv_up, grad_q, grad_kv)
        operands = [pltpu.with_memory_space_constraint(x, pltpu.HBM) for x in operands]
        hbm = pl.BlockSpec(memory_space=pltpu.HBM)

        vmem = pl.BlockSpec(memory_space=pltpu.VMEM)

        def like(x):
            return pltpu.VMEM(x.shape, x.dtype)

        moved = (
            pltpu.VMEM((n_t, rows, width), bf16),
            pltpu.VMEM((n_dp, *grad_q.shape), bf16),
            pltpu.VMEM((n_dp, *grad_kv.shape), bf16),
            pltpu.VMEM((devices, rows, part), bf16),
            *(like(x) for x in operands[:4]),
        )
        arrived = pl.pallas_call(
            functools.partial(exchange, n_dp, n_t),
            out_shape=moved,
            in_specs=[hbm] * len(operands),
            out_specs=(vmem,) * len(moved),
            scratch_shapes=[
                *(like(x) for x in operands[4:6]),
                pltpu.VMEM((n_dp, rows, part), bf16),
                like(moved[0]),
                pltpu.SemaphoreType.DMA((8,)),
                pltpu.SemaphoreType.DMA((4,)),
                pltpu.SemaphoreType.DMA((4,)),
            ],
            compiler_params=pltpu.CompilerParams(
                collective_id=0, has_side_effects=True, vmem_limit_bytes=LIMIT
            ),
        )(*operands)
        results = (
            jax.ShapeDtypeStruct((rows, q_width), f32),
            jax.ShapeDtypeStruct((rows, kv_width), f32),
            jax.ShapeDtypeStruct((q_part, grad_q.shape[1]), f32),
            jax.ShapeDtypeStruct((kv_part, grad_kv.shape[1]), f32),
        )
        arrived = [pltpu.with_memory_space_constraint(x, pltpu.VMEM) for x in arrived]
        return pl.pallas_call(
            finish,
            out_shape=results,
            in_specs=[vmem] * len(arrived),
            out_specs=(hbm,) * 4,
            scratch_shapes=[
                pltpu.VMEM((devices * rows, part), f32),
                *(like(x) for x in results),
                pltpu.SemaphoreType.DMA((4,)),
            ],
            compiler_params=pltpu.CompilerParams(vmem_limit_bytes=LIMIT),
        )(*arrived)

    return jax.shard_map(
        body,
        mesh=mesh,
        in_specs=(
            P(("dp", "tensor"), None),
            P(("dp", "tensor"), None),
            P(),
            P(),
            P(None, "tensor"),
            P(None, "tensor"),
            P("dp", "tensor"),
            P("dp", "tensor"),
        ),
        out_specs=(
            P(("dp", "tensor"), None),
            P(("dp", "tensor"), None),
            P("dp", "tensor"),
            P("dp", "tensor"),
        ),
        check_vma=False,
    )
```

```python
import functools

import jax
import jax.numpy as jnp
from jax import lax
from jax.experimental import pallas as pl
from jax.experimental.pallas import tpu as pltpu
from jax.sharding import PartitionSpec as P

EPS = 1e-06
UNROLL = 64
PIECES = 1
LIMIT = 24 * 1024 * 1024


def repeat(count, step):
    if count <= UNROLL:
        for index in range(count):
            step(index)
    else:

        def body(index, carry):
            step(index)
            return carry

        lax.fori_loop(0, count, body, 0)


def unit_rows(raw):
    values = raw.astype(jnp.float32)
    inverse = lax.rsqrt(jnp.mean(values * values, axis=-1, keepdims=True) + EPS)
    return values * inverse, inverse


def backward_of_norm(incoming, unit, inverse, gain):
    scaled = gain * incoming
    return inverse * (scaled - unit * jnp.mean(scaled * unit, axis=-1, keepdims=True))


def wait_bytes(ref, sem):
    pltpu.make_async_copy(ref, ref, sem).wait()


def exchange(
    n_dp, n_t,
    lq_hbm, lkv_hbm, gain_q_hbm, gain_kv_hbm, q_up_hbm, kv_up_hbm, gq_hbm, gkv_hbm,
    g_recv, all_gq, all_gkv, normed_recv, lq, lkv, gain_q, gain_kv,
    q_up, kv_up, normed_send, g_send,
    load_sem, send_sem, recv_sem, permit_sem,
):
    me_d, me_t = lax.axis_index("dp"), lax.axis_index("tensor")
    me = me_d * n_t + me_t
    devices = n_dp * n_t
    rows = lq.shape[0]
    q_width, kv_width = lq.shape[1], lkv.shape[1]
    q_part, kv_part = q_width // n_dp, kv_width // n_dp
    gq, gkv = all_gq.at[me_d], all_gkv.at[me_d]
    mesh = pl.DeviceIdType.MESH

    def depth(d, t):
        return t // 2 + t % 2 + d // 2

    everyone = [(d, t) for d in range(n_dp) for t in range(n_t)]
    everyone.sort(key=lambda place: depth(*place))
    deepest = depth(*everyone[-1])

    def remote(d, t):
        return depth(d, t) >= max(1, deepest - 1)

    def near(d, t):
        return depth(d, t) < max(1, deepest - 1)

    def first(d, t):
        return (t == 0) & (d < 2)

    def middle(d, t):
        return near(d, t) & ((t != 0) | (d >= 2))

    remotes = sum(int(remote(d, t)) for d, t in everyone)
    nears = devices - remotes
    am_near = near(me_d, me_t)
    am_remote = remote(me_d, me_t)
    am_last = depth(me_d, me_t) == deepest

    def each(group, skip, act):
        if devices <= UNROLL:
            for d, t in everyone:
                if not group(d, t):
                    continue
                if skip:
                    pl.when((me_d != d) | (me_t != t))(functools.partial(act, d, t))
                else:
                    act(d, t)
        else:

            def step(index, carry):
                d, t = lax.rem(index, n_dp), lax.div(index, n_dp)
                wanted = group(d, t)
                if skip:
                    wanted &= index != me_t * n_dp + me_d
                pl.when(wanted)(functools.partial(act, d, t))
                return carry

            lax.fori_loop(0, devices, step, 0)

    def line(count, mine, wanted, act):
        def step(index):
            pl.when((mine != index) & wanted(index))(functools.partial(act, index))

        repeat(count, step)

    loads = []
    for source, target, pieces in (
        (lq_hbm, lq, 1),
        (lkv_hbm, lkv, 1),
        (gain_q_hbm, gain_q, 1),
        (gain_kv_hbm, gain_kv, 1),
        (gq_hbm, gq, 1),
        (gkv_hbm, gkv, 1),
        (kv_up_hbm, kv_up, 1),
        (q_up_hbm, q_up, PIECES),
    ):
        size = source.shape[0] // pieces
        for piece in range(pieces):
            span = pl.ds(piece * size, size)
            loads.append(
                pltpu.make_async_copy(
                    source.at[span], target.at[span], load_sem.at[len(loads)]
                )
            )
    for load in loads:
        load.start()

    barrier = pltpu.get_barrier_semaphore()

    def greet(d, t):
        pl.semaphore_signal(barrier, inc=1, device_id=(d, t), device_id_type=mesh)

    pl.when(am_near)(functools.partial(each, near, True, greet))
    each(remote, True, greet)

    def send(source, target, kind, d, t):
        pltpu.make_async_remote_copy(
            src_ref=source,
            dst_ref=target,
            send_sem=send_sem.at[kind],
            recv_sem=recv_sem.at[kind],
            device_id=(d, t),
            device_id_type=mesh,
        ).start()

    def send_sums(d, t):
        send(g_send.at[t], g_recv.at[me_t], 0, d, t)

    def send_normed(d, t):
        send(normed_send.at[d], normed_recv.at[me], 1, d, t)

    def send_grads(d):
        send(gq, all_gq.at[me_d], 2, d, me_t)
        send(gkv, all_gkv.at[me_d], 3, d, me_t)

    def permit(d, t):
        pl.semaphore_signal(permit_sem, inc=1, device_id=(d, t), device_id_type=mesh)

    def sums_to(group):
        line(n_t, me_t, lambda t: group(me_d, t), lambda t: send_sums(me_d, t))

    def grads_to(group):
        line(n_dp, me_d, lambda d: group(d, me_t), send_grads)

    for load in loads[:4]:
        load.wait()
    normed_q = gain_q[...] * unit_rows(lq[...])[0]
    normed_kv = gain_kv[...] * unit_rows(lkv[...])[0]
    for d in range(n_dp):
        piece = jnp.concatenate(
            (
                normed_q[:, d * q_part : (d + 1) * q_part],
                normed_kv[:, d * kv_part : (d + 1) * kv_part],
            ),
            axis=1,
        )
        normed_send[d] = piece.astype(jnp.bfloat16)

    @pl.when(am_last)
    def _():
        pl.semaphore_wait(barrier, devices - 1)
        each(near, False, send_normed)
        each(near, False, permit)

    normed_recv[me] = normed_send[me_d]
    nt = (((1,), (1,)), ((), ()))
    for load in loads[4:7]:
        load.wait()
    g_kv = lax.dot_general(gkv[...], kv_up[...], nt, preferred_element_type=jnp.float32)
    for t in range(n_t):
        g_send[t, :, q_width:] = g_kv[t * rows : (t + 1) * rows].astype(g_send.dtype)
    size = q_width // PIECES
    for piece in range(PIECES):
        loads[7 + piece].wait()
        span = slice(piece * size, (piece + 1) * size)
        g_q = lax.dot_general(gq[...], q_up[span], nt, preferred_element_type=jnp.float32)
        for t in range(n_t):
            g_send[t, :, span] = g_q[t * rows : (t + 1) * rows].astype(g_send.dtype)
    g_recv[me_t] = g_send[me_t]

    @pl.when(am_near)
    def _():
        pl.semaphore_wait(barrier, nears - 1)
        each(first, True, send_normed)
        sums_to(first)
        each(middle, True, send_normed)
        sums_to(middle)
        grads_to(near)
        pl.semaphore_wait(permit_sem, remotes)
        each(remote, False, send_normed)
        sums_to(remote)
        grads_to(remote)

    @pl.when(am_remote)
    def _():
        @pl.when(jnp.logical_not(am_last))
        def _():
            pl.semaphore_wait(barrier, devices - 1)
            each(first, False, send_normed)

        sums_to(first)

        @pl.when(jnp.logical_not(am_last))
        def _():
            each(middle, False, send_normed)
            each(near, False, permit)

        sums_to(middle)
        each(remote, True, send_normed)
        sums_to(remote)
        grads_to(near)
        grads_to(remote)

    for sem in (recv_sem, send_sem):
        wait_bytes(all_gq.at[pl.ds(0, n_dp - 1)], sem.at[2])
        wait_bytes(all_gkv.at[pl.ds(0, n_dp - 1)], sem.at[3])
        wait_bytes(normed_recv.at[pl.ds(0, devices - 1)], sem.at[1])
        wait_bytes(g_recv.at[pl.ds(0, n_t - 1)], sem.at[0])


def finish(
    g, gq, gkv, normed_in, lq, lkv, gain_q, gain_kv,
    out_q_hbm, out_kv_hbm, d_q_hbm, d_kv_hbm,
    normed_all, out_q, out_kv, d_q, d_kv,
    store_sem,
):
    stores = [
        pltpu.make_async_copy(source, target, store_sem.at[index])
        for index, (source, target) in enumerate(
            ((d_q, d_q_hbm), (d_kv, d_kv_hbm), (out_q, out_q_hbm), (out_kv, out_kv_hbm))
        )
    ]
    n_t, rows = g.shape[:2]
    devices = normed_in.shape[0]
    q_width = lq.shape[1]
    q_part = d_q.shape[0]
    group = max(1, 8 // rows)

    def gather_rows(index):
        block = jnp.concatenate(
            [normed_in[index * group + k].astype(jnp.float32) for k in range(group)], axis=0
        )
        start = index * group * rows
        if not isinstance(start, int):
            start = pl.multiple_of(start, group * rows)
        normed_all[pl.ds(start, group * rows), :] = block

    repeat(devices // group, gather_rows)
    normed = normed_all[...].astype(jnp.bfloat16)
    tn = (((0,), (0,)), ((), ()))
    tokens = normed.shape[0]
    d_q[...] = lax.dot_general(
        normed[:, :q_part], gq[...].reshape(tokens, -1), tn, preferred_element_type=jnp.float32
    )
    stores[0].start()
    d_kv[...] = lax.dot_general(
        normed[:, q_part:], gkv[...].reshape(tokens, -1), tn, preferred_element_type=jnp.float32
    )
    stores[1].start()
    total = g[0].astype(jnp.float32)
    for t in range(1, n_t):
        total += g[t].astype(jnp.float32)
    out_q[...] = backward_of_norm(total[:, :q_width], *unit_rows(lq[...]), gain_q[...])
    stores[2].start()
    out_kv[...] = backward_of_norm(total[:, q_width:], *unit_rows(lkv[...]), gain_kv[...])
    stores[3].start()
    for store in stores:
        store.wait()


def solution(mesh):
    n_dp, n_t = mesh.shape["dp"], mesh.shape["tensor"]

    def body(latent_q, latent_kv, gain_q, gain_kv, q_up, kv_up, grad_q, grad_kv):
        rows, q_width = latent_q.shape
        kv_width = latent_kv.shape[1]
        q_part, kv_part = q_width // n_dp, kv_width // n_dp
        part = q_part + kv_part
        width = q_width + kv_width
        devices = n_dp * n_t
        f32, bf16 = jnp.float32, jnp.bfloat16
        operands = (latent_q, latent_kv, gain_q, gain_kv, q_up, kv_up, grad_q, grad_kv)
        operands = [pltpu.with_memory_space_constraint(x, pltpu.HBM) for x in operands]
        hbm = pl.BlockSpec(memory_space=pltpu.HBM)

        vmem = pl.BlockSpec(memory_space=pltpu.VMEM)

        def like(x):
            return pltpu.VMEM(x.shape, x.dtype)

        moved = (
            pltpu.VMEM((n_t, rows, width), bf16),
            pltpu.VMEM((n_dp, *grad_q.shape), bf16),
            pltpu.VMEM((n_dp, *grad_kv.shape), bf16),
            pltpu.VMEM((devices, rows, part), bf16),
            *(like(x) for x in operands[:4]),
        )
        arrived = pl.pallas_call(
            functools.partial(exchange, n_dp, n_t),
            out_shape=moved,
            in_specs=[hbm] * len(operands),
            out_specs=(vmem,) * len(moved),
            scratch_shapes=[
                *(like(x) for x in operands[4:6]),
                pltpu.VMEM((n_dp, rows, part), bf16),
                like(moved[0]),
                pltpu.SemaphoreType.DMA((7 + PIECES,)),
                pltpu.SemaphoreType.DMA((4,)),
                pltpu.SemaphoreType.DMA((4,)),
                pltpu.SemaphoreType.REGULAR,
            ],
            compiler_params=pltpu.CompilerParams(
                collective_id=0, has_side_effects=True, vmem_limit_bytes=LIMIT
            ),
        )(*operands)
        results = (
            jax.ShapeDtypeStruct((rows, q_width), f32),
            jax.ShapeDtypeStruct((rows, kv_width), f32),
            jax.ShapeDtypeStruct((q_part, grad_q.shape[1]), f32),
            jax.ShapeDtypeStruct((kv_part, grad_kv.shape[1]), f32),
        )
        arrived = [pltpu.with_memory_space_constraint(x, pltpu.VMEM) for x in arrived]
        return pl.pallas_call(
            finish,
            out_shape=results,
            in_specs=[vmem] * len(arrived),
            out_specs=(hbm,) * 4,
            scratch_shapes=[
                pltpu.VMEM((devices * rows, part), f32),
                *(like(x) for x in results),
                pltpu.SemaphoreType.DMA((4,)),
            ],
            compiler_params=pltpu.CompilerParams(vmem_limit_bytes=LIMIT),
        )(*arrived)

    return jax.shard_map(
        body,
        mesh=mesh,
        in_specs=(
            P(("dp", "tensor"), None),
            P(("dp", "tensor"), None),
            P(),
            P(),
            P(None, "tensor"),
            P(None, "tensor"),
            P("dp", "tensor"),
            P("dp", "tensor"),
        ),
        out_specs=(
            P(("dp", "tensor"), None),
            P(("dp", "tensor"), None),
            P("dp", "tensor"),
            P("dp", "tensor"),
        ),
        check_vma=False,
    )
```

```python
import functools

import jax
import jax.numpy as jnp
from jax import lax
from jax.experimental import pallas as pl
from jax.experimental.pallas import tpu as pltpu
from jax.sharding import PartitionSpec as P

EPS = 1e-06
UNROLL = 64
LIMIT = 24 * 1024 * 1024


def repeat(count, step):
    if count <= UNROLL:
        for index in range(count):
            step(index)
    else:

        def body(index, carry):
            step(index)
            return carry

        lax.fori_loop(0, count, body, 0)


def unit_rows(raw):
    values = raw.astype(jnp.float32)
    inverse = lax.rsqrt(jnp.mean(values * values, axis=-1, keepdims=True) + EPS)
    return values * inverse, inverse


def backward_of_norm(incoming, unit, inverse, gain):
    scaled = gain * incoming
    return inverse * (scaled - unit * jnp.mean(scaled * unit, axis=-1, keepdims=True))


def weight_gradient(target, normed_all, all_grads, rows, columns):
    tokens = normed_all.shape[0]
    target[...] = lax.dot_general(
        normed_all[:, rows].astype(jnp.bfloat16),
        all_grads[:, :, columns].reshape(tokens, -1),
        (((0,), (0,)), ((), ())),
        preferred_element_type=jnp.float32,
    )


def wait_bytes(ref, sem):
    pltpu.make_async_copy(ref, ref, sem).wait()


def exchange(
    n_dp, n_t,
    lq_hbm, lkv_hbm, gain_q_hbm, gain_kv_hbm, q_up_hbm, kv_up_hbm, gq_hbm, gkv_hbm,
    g_recv, all_grads, normed_all, unit_q, unit_kv, inverse_q, inverse_kv, gain_q, gain_kv, d_q,
    lq, lkv, normed_recv, q_up, kv_up, normed_send, g_send,
    recv_sem,
):
    me_d, me_t = lax.axis_index("dp"), lax.axis_index("tensor")
    me = me_d * n_t + me_t
    devices = n_dp * n_t
    rows = lq.shape[0]
    q_width, kv_width = lq.shape[1], lkv.shape[1]
    q_part, kv_part = q_width // n_dp, kv_width // n_dp
    q_cols = q_up.shape[1]
    grads = all_grads.at[me_d]
    gq, gkv = grads.at[:, :q_cols], grads.at[:, q_cols:]
    mesh = pl.DeviceIdType.MESH

    def depth(d, t):
        return t // 2 + t % 2 + d // 2

    everyone = [(d, t) for d in range(n_dp) for t in range(n_t)]
    everyone.sort(key=lambda place: depth(*place))
    deepest = depth(*everyone[-1])

    def remote(d, t):
        return depth(d, t) >= max(1, deepest - 1)

    def near(d, t):
        return depth(d, t) < max(1, deepest - 1)

    def first(d, t):
        return (t == 0) & (d < 2)

    def middle(d, t):
        return near(d, t) & ((t != 0) | (d >= 2))

    remotes = sum(int(remote(d, t)) for d, t in everyone)
    nears = devices - remotes
    am_near = near(me_d, me_t)
    am_remote = remote(me_d, me_t)
    am_last = depth(me_d, me_t) == deepest

    def each(group, skip, act):
        if devices <= UNROLL:
            for d, t in everyone:
                if not group(d, t):
                    continue
                if skip:
                    pl.when((me_d != d) | (me_t != t))(functools.partial(act, d, t))
                else:
                    act(d, t)
        else:

            def step(index, carry):
                d, t = lax.rem(index, n_dp), lax.div(index, n_dp)
                wanted = group(d, t)
                if skip:
                    wanted &= index != me_t * n_dp + me_d
                pl.when(wanted)(functools.partial(act, d, t))
                return carry

            lax.fori_loop(0, devices, step, 0)

    def line(count, mine, wanted, act):
        def step(index):
            pl.when((mine != index) & wanted(index))(functools.partial(act, index))

        repeat(count, step)

    half = n_t // 2
    my_half = me_t // half
    group = max(1, 8 // rows)
    blocks = half // group

    def gather_rows(which, index):
        d, start = index // blocks, which * half + index % blocks * group
        source = d * n_t + start
        block = jnp.concatenate(
            [normed_recv[source + k].astype(jnp.float32) for k in range(group)], axis=0
        )
        start = source * rows
        if not isinstance(start, int):
            start = pl.multiple_of(start, group * rows)
        normed_all[pl.ds(start, group * rows), :] = block

    def talk(load_sem, send_sem, permit_sem):
        loads = [
            pltpu.make_async_copy(source, target, load_sem.at[index])
            for index, (source, target) in enumerate(
                (
                    (lq_hbm, lq),
                    (lkv_hbm, lkv),
                    (gain_q_hbm, gain_q),
                    (gain_kv_hbm, gain_kv),
                    (gkv_hbm, gkv),
                    (kv_up_hbm, kv_up),
                    (gq_hbm, gq),
                    (q_up_hbm, q_up),
                )
            )
        ]
        for load in loads:
            load.start()

        barrier = pltpu.get_barrier_semaphore()

        def greet(d, t):
            pl.semaphore_signal(barrier, inc=1, device_id=(d, t), device_id_type=mesh)

        pl.when(am_near)(functools.partial(each, near, True, greet))
        each(remote, True, greet)

        def send(source, target, kind, arrival, d, t):
            pltpu.make_async_remote_copy(
                src_ref=source,
                dst_ref=target,
                send_sem=send_sem.at[kind],
                recv_sem=recv_sem.at[arrival],
                device_id=(d, t),
                device_id_type=mesh,
            ).start()

        def send_sums(t):
            send(g_send.at[t], g_recv.at[me_t], 0, 0, me_d, t)

        def send_grads(d):
            send(grads, grads, 1, 1, d, me_t)

        def send_normed(d, t):
            send(normed_send.at[d], normed_recv.at[me], 2, 2 + my_half, d, t)

        def permit(d, t):
            pl.semaphore_signal(permit_sem, inc=1, device_id=(d, t), device_id_type=mesh)

        def sums_to(group):
            line(n_t, me_t, lambda t: group(me_d, t), send_sums)

        def grads_to(group):
            line(n_dp, me_d, lambda d: group(d, me_t), send_grads)

        for load in loads[:4]:
            load.wait()
        unit_q[...], inverse = unit_rows(lq[...])
        inverse_q[...] = jnp.broadcast_to(inverse, inverse_q.shape)
        unit_kv[...], inverse = unit_rows(lkv[...])
        inverse_kv[...] = jnp.broadcast_to(inverse, inverse_kv.shape)
        normed_q = gain_q[...] * unit_q[...]
        normed_kv = gain_kv[...] * unit_kv[...]
        for d in range(n_dp):
            piece = jnp.concatenate(
                (
                    normed_q[:, d * q_part : (d + 1) * q_part],
                    normed_kv[:, d * kv_part : (d + 1) * kv_part],
                ),
                axis=1,
            )
            normed_send[d] = piece.astype(jnp.bfloat16)

        @pl.when(am_last)
        def _():
            pl.semaphore_wait(barrier, devices - 1)
            each(first, False, send_normed)
            each(near, False, permit)
            each(middle, False, send_normed)

        normed_recv[me] = normed_send[me_d]
        nt = (((1,), (1,)), ((), ()))

        def partial_sums(needed, cotangent, weights, start):
            for load in needed:
                load.wait()
            sums = lax.dot_general(
                cotangent[...], weights[...], nt, preferred_element_type=jnp.float32
            )
            span = slice(start, start + sums.shape[1])
            for t in range(n_t):
                g_send[t, :, span] = sums[t * rows : (t + 1) * rows].astype(g_send.dtype)

        partial_sums(loads[4:6], gkv, kv_up, q_width)

        @pl.when(am_remote & jnp.logical_not(am_last))
        def _():
            pl.semaphore_wait(barrier, devices - 1)
            each(first, False, send_normed)
            each(near, False, permit)

        partial_sums(loads[6:], gq, q_up, 0)
        g_recv[me_t] = g_send[me_t]

        @pl.when(am_near)
        def _():
            pl.semaphore_wait(barrier, nears - 1)
            each(first, True, send_normed)
            sums_to(first)
            each(middle, True, send_normed)
            sums_to(middle)
            grads_to(near)
            pl.semaphore_wait(permit_sem, remotes)
            each(remote, False, send_normed)
            sums_to(remote)
            grads_to(remote)

        @pl.when(am_remote)
        def _():
            sums_to(first)

            @pl.when(jnp.logical_not(am_last))
            def _():
                each(middle, False, send_normed)

            sums_to(middle)
            each(remote, True, send_normed)
            sums_to(remote)
            grads_to(near)
            grads_to(remote)

        wait_bytes(g_recv.at[pl.ds(0, n_t - 1)], send_sem.at[0])
        wait_bytes(all_grads.at[pl.ds(0, n_dp - 1)], send_sem.at[1])
        wait_bytes(normed_recv.at[pl.ds(0, devices - 1)], send_sem.at[2])

    pl.run_scoped(
        talk,
        pltpu.SemaphoreType.DMA((8,)),
        pltpu.SemaphoreType.DMA((3,)),
        pltpu.SemaphoreType.REGULAR,
    )
    wait_bytes(all_grads.at[pl.ds(0, n_dp - 1)], recv_sem.at[1])
    for which in range(2):
        count = n_dp * half

        @pl.when(my_half == which)
        def _():
            wait_bytes(normed_recv.at[pl.ds(0, count - 1)], recv_sem.at[2 + which])

        @pl.when(my_half != which)
        def _():
            wait_bytes(normed_recv.at[pl.ds(0, count)], recv_sem.at[2 + which])

        repeat(n_dp * blocks, functools.partial(gather_rows, which))

    weight_gradient(d_q, normed_all, all_grads, slice(0, q_part), slice(0, q_cols))
    wait_bytes(g_recv.at[pl.ds(0, n_t - 1)], recv_sem.at[0])


def finish(
    g, all_grads, normed_all, unit_q, unit_kv, inverse_q, inverse_kv, gain_q, gain_kv, d_q,
    out_q_hbm, out_kv_hbm, d_q_hbm, d_kv_hbm,
    out_q, out_kv, d_kv,
    store_sem,
):
    stores = []

    def store(source, target):
        stores.append(pltpu.make_async_copy(source, target, store_sem.at[len(stores)]))
        stores[-1].start()

    store(d_q, d_q_hbm)
    n_t = g.shape[0]
    q_width = unit_q.shape[1]
    q_part, q_cols = d_q.shape
    weight_gradient(d_kv, normed_all, all_grads, slice(q_part, None), slice(q_cols, None))
    store(d_kv, d_kv_hbm)
    total = g[0].astype(jnp.float32)
    for t in range(1, n_t):
        total += g[t].astype(jnp.float32)
    out_q[...] = backward_of_norm(total[:, :q_width], unit_q[...], inverse_q[...], gain_q[...])
    out_kv[...] = backward_of_norm(total[:, q_width:], unit_kv[...], inverse_kv[...], gain_kv[...])
    store(out_q, out_q_hbm)
    store(out_kv, out_kv_hbm)
    for copy in stores:
        copy.wait()


def solution(mesh):
    n_dp, n_t = mesh.shape["dp"], mesh.shape["tensor"]

    def body(latent_q, latent_kv, gain_q, gain_kv, q_up, kv_up, grad_q, grad_kv):
        rows, q_width = latent_q.shape
        kv_width = latent_kv.shape[1]
        q_part, kv_part = q_width // n_dp, kv_width // n_dp
        part = q_part + kv_part
        width = q_width + kv_width
        devices = n_dp * n_t
        f32, bf16 = jnp.float32, jnp.bfloat16
        operands = (latent_q, latent_kv, gain_q, gain_kv, q_up, kv_up, grad_q, grad_kv)
        operands = [pltpu.with_memory_space_constraint(x, pltpu.HBM) for x in operands]
        hbm = pl.BlockSpec(memory_space=pltpu.HBM)

        vmem = pl.BlockSpec(memory_space=pltpu.VMEM)

        def like(x):
            return pltpu.VMEM(x.shape, x.dtype)

        results = (
            jax.ShapeDtypeStruct((rows, q_width), f32),
            jax.ShapeDtypeStruct((rows, kv_width), f32),
            jax.ShapeDtypeStruct((q_part, grad_q.shape[1]), f32),
            jax.ShapeDtypeStruct((kv_part, grad_kv.shape[1]), f32),
        )
        passed = (
            pltpu.VMEM((n_t, rows, width), bf16),
            pltpu.VMEM((n_dp, grad_q.shape[0], grad_q.shape[1] + grad_kv.shape[1]), bf16),
            pltpu.VMEM((devices * rows, part), f32),
            *(like(x) for x in results[:2] * 2),
            like(gain_q),
            like(gain_kv),
            like(results[2]),
        )
        arrived = pl.pallas_call(
            functools.partial(exchange, n_dp, n_t),
            out_shape=passed,
            in_specs=[hbm] * len(operands),
            out_specs=(vmem,) * len(passed),
            scratch_shapes=[
                like(latent_q),
                like(latent_kv),
                pltpu.VMEM((devices, rows, part), bf16),
                *(like(x) for x in operands[4:6]),
                pltpu.VMEM((n_dp, rows, part), bf16),
                like(passed[0]),
                pltpu.SemaphoreType.DMA((4,)),
            ],
            compiler_params=pltpu.CompilerParams(
                collective_id=0, has_side_effects=True, vmem_limit_bytes=LIMIT
            ),
        )(*operands)
        arrived = [pltpu.with_memory_space_constraint(x, pltpu.VMEM) for x in arrived]
        return pl.pallas_call(
            finish,
            out_shape=results,
            in_specs=[vmem] * len(arrived),
            out_specs=(hbm,) * 4,
            scratch_shapes=[
                *(like(x) for x in (*results[:2], results[3])),
                pltpu.SemaphoreType.DMA((4,)),
            ],
            compiler_params=pltpu.CompilerParams(vmem_limit_bytes=LIMIT),
        )(*arrived)

    return jax.shard_map(
        body,
        mesh=mesh,
        in_specs=(
            P(("dp", "tensor"), None),
            P(("dp", "tensor"), None),
            P(),
            P(),
            P(None, "tensor"),
            P(None, "tensor"),
            P("dp", "tensor"),
            P("dp", "tensor"),
        ),
        out_specs=(
            P(("dp", "tensor"), None),
            P(("dp", "tensor"), None),
            P("dp", "tensor"),
            P("dp", "tensor"),
        ),
        check_vma=False,
    )
```

```python
import functools

import jax
import jax.numpy as jnp
from jax import lax
from jax.experimental import pallas as pl
from jax.experimental.pallas import tpu as pltpu
from jax.sharding import PartitionSpec as P

EPS = 1e-06
UNROLL = 64
LIMIT = 24 * 1024 * 1024


def repeat(count, step):
    if count <= UNROLL:
        for index in range(count):
            step(index)
    else:

        def body(index, carry):
            step(index)
            return carry

        lax.fori_loop(0, count, body, 0)


def unit_rows(raw):
    values = raw.astype(jnp.float32)
    inverse = lax.rsqrt(jnp.mean(values * values, axis=-1, keepdims=True) + EPS)
    return values * inverse, inverse


def backward_of_norm(incoming, unit, inverse, gain):
    scaled = gain * incoming
    return inverse * (scaled - unit * jnp.mean(scaled * unit, axis=-1, keepdims=True))


def weight_gradient(target, normed_all, all_grads, rows, columns):
    tokens = normed_all.shape[0]
    target[...] = lax.dot_general(
        normed_all[:, rows].astype(jnp.bfloat16),
        all_grads[:, :, columns].reshape(tokens, -1),
        (((0,), (0,)), ((), ())),
        preferred_element_type=jnp.float32,
    )


def wait_bytes(ref, sem):
    pltpu.make_async_copy(ref, ref, sem).wait()


def exchange(
    n_dp, n_t,
    lq_hbm, lkv_hbm, gain_q_hbm, gain_kv_hbm, q_up_hbm, kv_up_hbm, gq_hbm, gkv_hbm,
    g_recv, all_grads, normed_all, unit_q, unit_kv, inverse_q, inverse_kv, gain_q, gain_kv, d_q, d_kv,
    lq, lkv, normed_recv, q_up, kv_up, normed_send, g_send,
    recv_sem,
):
    me_d, me_t = lax.axis_index("dp"), lax.axis_index("tensor")
    me = me_d * n_t + me_t
    devices = n_dp * n_t
    rows = lq.shape[0]
    q_width, kv_width = lq.shape[1], lkv.shape[1]
    q_part, kv_part = q_width // n_dp, kv_width // n_dp
    q_cols = q_up.shape[1]
    grads = all_grads.at[me_d]
    gq, gkv = grads.at[:, :q_cols], grads.at[:, q_cols:]
    mesh = pl.DeviceIdType.MESH

    def depth(d, t):
        return t // 2 + t % 2 + d // 2

    everyone = [(d, t) for d in range(n_dp) for t in range(n_t)]
    everyone.sort(key=lambda place: depth(*place))
    deepest = depth(*everyone[-1])

    def remote(d, t):
        return depth(d, t) >= max(1, deepest - 1)

    def near(d, t):
        return depth(d, t) < max(1, deepest - 1)

    def first(d, t):
        return (t == 0) & (d < 2)

    def middle(d, t):
        return near(d, t) & ((t != 0) | (d >= 2))

    remotes = sum(int(remote(d, t)) for d, t in everyone)
    nears = devices - remotes
    am_first = first(me_d, me_t)
    am_near = near(me_d, me_t)
    am_remote = remote(me_d, me_t)
    am_last = depth(me_d, me_t) == deepest

    def each(group, skip, act):
        if devices <= UNROLL:
            for d, t in everyone:
                if not group(d, t):
                    continue
                if skip:
                    pl.when((me_d != d) | (me_t != t))(functools.partial(act, d, t))
                else:
                    act(d, t)
        else:

            def step(index, carry):
                d, t = lax.rem(index, n_dp), lax.div(index, n_dp)
                wanted = group(d, t)
                if skip:
                    wanted &= index != me_t * n_dp + me_d
                pl.when(wanted)(functools.partial(act, d, t))
                return carry

            lax.fori_loop(0, devices, step, 0)

    def line(count, mine, wanted, act):
        def step(index):
            pl.when((mine != index) & wanted(index))(functools.partial(act, index))

        repeat(count, step)

    half = n_t // 2
    my_half = me_t // half
    group = max(1, 8 // rows)
    blocks = half // group

    def gather_rows(which, index):
        d, start = index // blocks, which * half + index % blocks * group
        source = d * n_t + start
        block = jnp.concatenate(
            [normed_recv[source + k].astype(jnp.float32) for k in range(group)], axis=0
        )
        start = source * rows
        if not isinstance(start, int):
            start = pl.multiple_of(start, group * rows)
        normed_all[pl.ds(start, group * rows), :] = block

    def talk(load_sem, send_sem, permit_sem):
        loads = [
            pltpu.make_async_copy(source, target, load_sem.at[index])
            for index, (source, target) in enumerate(
                (
                    (lq_hbm, lq),
                    (lkv_hbm, lkv),
                    (gain_q_hbm, gain_q),
                    (gain_kv_hbm, gain_kv),
                    (gkv_hbm, gkv),
                    (kv_up_hbm, kv_up),
                    (gq_hbm, gq),
                    (q_up_hbm, q_up),
                )
            )
        ]
        for load in loads:
            load.start()

        barrier = pltpu.get_barrier_semaphore()

        def greet(d, t):
            pl.semaphore_signal(barrier, inc=1, device_id=(d, t), device_id_type=mesh)

        pl.when(am_near)(functools.partial(each, near, True, greet))
        each(remote, True, greet)

        def send(source, target, kind, arrival, d, t):
            pltpu.make_async_remote_copy(
                src_ref=source,
                dst_ref=target,
                send_sem=send_sem.at[kind],
                recv_sem=recv_sem.at[arrival],
                device_id=(d, t),
                device_id_type=mesh,
            ).start()

        def send_sums(t):
            send(g_send.at[t], g_recv.at[me_t], 0, 0, me_d, t)

        def send_grads(d):
            send(grads, grads, 1, 1, d, me_t)

        def send_normed(d, t):
            send(normed_send.at[d], normed_recv.at[me], 2, 2 + my_half, d, t)

        def permit(d, t):
            pl.semaphore_signal(permit_sem, inc=1, device_id=(d, t), device_id_type=mesh)

        def sums_to(group):
            line(n_t, me_t, lambda t: group(me_d, t), send_sums)

        def grads_to(group):
            line(n_dp, me_d, lambda d: group(d, me_t), send_grads)

        @pl.when(am_first)
        def _():
            pl.semaphore_wait(barrier, nears - 1)

        for load in loads[:4]:
            load.wait()
        unit_q[...], inverse = unit_rows(lq[...])
        inverse_q[...] = jnp.broadcast_to(inverse, inverse_q.shape)
        unit_kv[...], inverse = unit_rows(lkv[...])
        inverse_kv[...] = jnp.broadcast_to(inverse, inverse_kv.shape)
        normed_q = gain_q[...] * unit_q[...]
        normed_kv = gain_kv[...] * unit_kv[...]
        for d in range(n_dp):
            piece = jnp.concatenate(
                (
                    normed_q[:, d * q_part : (d + 1) * q_part],
                    normed_kv[:, d * kv_part : (d + 1) * kv_part],
                ),
                axis=1,
            )
            normed_send[d] = piece.astype(jnp.bfloat16)

        @pl.when(am_last)
        def _():
            pl.semaphore_wait(barrier, devices - 1)
            each(first, False, send_normed)
            each(near, False, permit)
            each(middle, False, send_normed)

        normed_recv[me] = normed_send[me_d]
        nt = (((1,), (1,)), ((), ()))

        def partial_sums(needed, cotangent, weights, start):
            for load in needed:
                load.wait()
            sums = lax.dot_general(
                cotangent[...], weights[...], nt, preferred_element_type=jnp.float32
            )
            span = slice(start, start + sums.shape[1])
            for t in range(n_t):
                g_send[t, :, span] = sums[t * rows : (t + 1) * rows].astype(g_send.dtype)

        partial_sums(loads[4:6], gkv, kv_up, q_width)

        @pl.when(am_remote & jnp.logical_not(am_last))
        def _():
            pl.semaphore_wait(barrier, devices - 1)
            each(first, False, send_normed)
            each(near, False, permit)

        partial_sums(loads[6:], gq, q_up, 0)
        g_recv[me_t] = g_send[me_t]

        @pl.when(am_near)
        def _():
            pl.when(jnp.logical_not(am_first))(lambda: pl.semaphore_wait(barrier, nears - 1))
            each(first, True, send_normed)
            sums_to(first)
            each(middle, True, send_normed)
            sums_to(middle)
            grads_to(near)
            pl.semaphore_wait(permit_sem, remotes)
            each(remote, False, send_normed)
            sums_to(remote)
            grads_to(remote)

        @pl.when(am_remote)
        def _():
            sums_to(first)

            @pl.when(jnp.logical_not(am_last))
            def _():
                each(middle, False, send_normed)

            sums_to(middle)
            each(remote, True, send_normed)
            sums_to(remote)
            grads_to(near)
            grads_to(remote)

        wait_bytes(all_grads.at[pl.ds(0, n_dp - 1)], recv_sem.at[1])
        for which in range(2):
            count = n_dp * half

            @pl.when(my_half == which)
            def _():
                wait_bytes(normed_recv.at[pl.ds(0, count - 1)], recv_sem.at[2 + which])

            @pl.when(my_half != which)
            def _():
                wait_bytes(normed_recv.at[pl.ds(0, count)], recv_sem.at[2 + which])

            repeat(n_dp * blocks, functools.partial(gather_rows, which))

        weight_gradient(d_q, normed_all, all_grads, slice(0, q_part), slice(0, q_cols))
        weight_gradient(d_kv, normed_all, all_grads, slice(q_part, None), slice(q_cols, None))
        wait_bytes(g_recv.at[pl.ds(0, n_t - 1)], send_sem.at[0])
        wait_bytes(all_grads.at[pl.ds(0, n_dp - 1)], send_sem.at[1])
        wait_bytes(normed_recv.at[pl.ds(0, devices - 1)], send_sem.at[2])

    pl.run_scoped(
        talk,
        pltpu.SemaphoreType.DMA((8,)),
        pltpu.SemaphoreType.DMA((3,)),
        pltpu.SemaphoreType.REGULAR,
    )
    wait_bytes(g_recv.at[pl.ds(0, n_t - 1)], recv_sem.at[0])


def finish(
    g, all_grads, normed_all, unit_q, unit_kv, inverse_q, inverse_kv, gain_q, gain_kv, d_q, d_kv,
    out_q_hbm, out_kv_hbm, d_q_hbm, d_kv_hbm,
    out_q, out_kv,
    store_sem,
):
    stores = []

    def store(source, target):
        stores.append(pltpu.make_async_copy(source, target, store_sem.at[len(stores)]))
        stores[-1].start()

    store(d_q, d_q_hbm)
    n_t = g.shape[0]
    q_width = unit_q.shape[1]
    store(d_kv, d_kv_hbm)
    total = g[0].astype(jnp.float32)
    for t in range(1, n_t):
        total += g[t].astype(jnp.float32)
    out_q[...] = backward_of_norm(total[:, :q_width], unit_q[...], inverse_q[...], gain_q[...])
    out_kv[...] = backward_of_norm(total[:, q_width:], unit_kv[...], inverse_kv[...], gain_kv[...])
    store(out_q, out_q_hbm)
    store(out_kv, out_kv_hbm)
    for copy in stores:
        copy.wait()


def solution(mesh):
    n_dp, n_t = mesh.shape["dp"], mesh.shape["tensor"]

    def body(latent_q, latent_kv, gain_q, gain_kv, q_up, kv_up, grad_q, grad_kv):
        rows, q_width = latent_q.shape
        kv_width = latent_kv.shape[1]
        q_part, kv_part = q_width // n_dp, kv_width // n_dp
        part = q_part + kv_part
        width = q_width + kv_width
        devices = n_dp * n_t
        f32, bf16 = jnp.float32, jnp.bfloat16
        operands = (latent_q, latent_kv, gain_q, gain_kv, q_up, kv_up, grad_q, grad_kv)
        operands = [pltpu.with_memory_space_constraint(x, pltpu.HBM) for x in operands]
        hbm = pl.BlockSpec(memory_space=pltpu.HBM)

        vmem = pl.BlockSpec(memory_space=pltpu.VMEM)

        def like(x):
            return pltpu.VMEM(x.shape, x.dtype)

        results = (
            jax.ShapeDtypeStruct((rows, q_width), f32),
            jax.ShapeDtypeStruct((rows, kv_width), f32),
            jax.ShapeDtypeStruct((q_part, grad_q.shape[1]), f32),
            jax.ShapeDtypeStruct((kv_part, grad_kv.shape[1]), f32),
        )
        passed = (
            pltpu.VMEM((n_t, rows, width), bf16),
            pltpu.VMEM((n_dp, grad_q.shape[0], grad_q.shape[1] + grad_kv.shape[1]), bf16),
            pltpu.VMEM((devices * rows, part), f32),
            *(like(x) for x in results[:2] * 2),
            like(gain_q),
            like(gain_kv),
            like(results[2]),
            like(results[3]),
        )
        arrived = pl.pallas_call(
            functools.partial(exchange, n_dp, n_t),
            out_shape=passed,
            in_specs=[hbm] * len(operands),
            out_specs=(vmem,) * len(passed),
            scratch_shapes=[
                like(latent_q),
                like(latent_kv),
                pltpu.VMEM((devices, rows, part), bf16),
                *(like(x) for x in operands[4:6]),
                pltpu.VMEM((n_dp, rows, part), bf16),
                like(passed[0]),
                pltpu.SemaphoreType.DMA((4,)),
            ],
            compiler_params=pltpu.CompilerParams(
                collective_id=0, has_side_effects=True, vmem_limit_bytes=LIMIT
            ),
        )(*operands)
        arrived = [pltpu.with_memory_space_constraint(x, pltpu.VMEM) for x in arrived]
        return pl.pallas_call(
            finish,
            out_shape=results,
            in_specs=[vmem] * len(arrived),
            out_specs=(hbm,) * 4,
            scratch_shapes=[
                *(like(x) for x in results[:2]),
                pltpu.SemaphoreType.DMA((4,)),
            ],
            compiler_params=pltpu.CompilerParams(vmem_limit_bytes=LIMIT),
        )(*arrived)

    return jax.shard_map(
        body,
        mesh=mesh,
        in_specs=(
            P(("dp", "tensor"), None),
            P(("dp", "tensor"), None),
            P(),
            P(),
            P(None, "tensor"),
            P(None, "tensor"),
            P("dp", "tensor"),
            P("dp", "tensor"),
        ),
        out_specs=(
            P(("dp", "tensor"), None),
            P(("dp", "tensor"), None),
            P("dp", "tensor"),
            P("dp", "tensor"),
        ),
        check_vma=False,
    )
```

```python
import functools

import jax
import jax.numpy as jnp
from jax import lax
from jax.experimental import pallas as pl
from jax.experimental.pallas import tpu as pltpu
from jax.sharding import PartitionSpec as P

EPS = 1e-06
UNROLL = 64
LIMIT = 24 * 1024 * 1024


def repeat(count, step):
    if count <= UNROLL:
        for index in range(count):
            step(index)
    else:

        def body(index, carry):
            step(index)
            return carry

        lax.fori_loop(0, count, body, 0)


def unit_rows(raw):
    values = raw.astype(jnp.float32)
    inverse = lax.rsqrt(jnp.mean(values * values, axis=-1, keepdims=True) + EPS)
    return values * inverse, inverse


def backward_of_norm(incoming, unit, inverse, gain):
    scaled = gain * incoming
    return inverse * (scaled - unit * jnp.mean(scaled * unit, axis=-1, keepdims=True))


def weight_gradient(target, normed_all, all_grads, rows, columns):
    tokens = normed_all.shape[0]
    target[...] = lax.dot_general(
        normed_all[:, rows].astype(jnp.bfloat16),
        all_grads[:, :, columns].reshape(tokens, -1),
        (((0,), (0,)), ((), ())),
        preferred_element_type=jnp.float32,
    )


def wait_bytes(ref, sem):
    pltpu.make_async_copy(ref, ref, sem).wait()


def exchange(
    n_dp, n_t,
    lq_hbm, lkv_hbm, gain_q_hbm, gain_kv_hbm, q_up_hbm, kv_up_hbm, gq_hbm, gkv_hbm,
    g_recv, all_grads, normed_all, unit_q, unit_kv, inverse_q, inverse_kv, gain_q, gain_kv, d_q, d_kv,
    lq, lkv, normed_recv, q_up, kv_up, normed_send, g_send,
):
    def talk(load_sem, send_sem, recv_sem, permit_sem):
        loads = []

        def fetch(*pairs):
            for source, target in pairs:
                loads.append(pltpu.make_async_copy(source, target, load_sem.at[len(loads)]))
                loads[-1].start()

        fetch((lq_hbm, lq), (lkv_hbm, lkv), (gain_q_hbm, gain_q), (gain_kv_hbm, gain_kv))
        me_d, me_t = lax.axis_index("dp"), lax.axis_index("tensor")
        me = me_d * n_t + me_t
        devices = n_dp * n_t
        rows = lq.shape[0]
        q_width, kv_width = lq.shape[1], lkv.shape[1]
        q_part, kv_part = q_width // n_dp, kv_width // n_dp
        q_cols = q_up.shape[1]
        grads = all_grads.at[me_d]
        gq, gkv = grads.at[:, :q_cols], grads.at[:, q_cols:]
        mesh = pl.DeviceIdType.MESH

        def depth(d, t):
            return t // 2 + t % 2 + d // 2

        everyone = [(d, t) for d in range(n_dp) for t in range(n_t)]
        everyone.sort(key=lambda place: depth(*place))
        deepest = depth(*everyone[-1])

        def remote(d, t):
            return depth(d, t) >= max(1, deepest - 1)

        def near(d, t):
            return depth(d, t) < max(1, deepest - 1)

        def first(d, t):
            return (t == 0) & (d < 2)

        def middle(d, t):
            return near(d, t) & ((t != 0) | (d >= 2))

        remotes = sum(int(remote(d, t)) for d, t in everyone)
        nears = devices - remotes
        am_first = first(me_d, me_t)
        am_near = near(me_d, me_t)
        am_remote = remote(me_d, me_t)
        am_last = depth(me_d, me_t) == deepest

        def each(group, skip, act):
            if devices <= UNROLL:
                for d, t in everyone:
                    if not group(d, t):
                        continue
                    if skip:
                        pl.when((me_d != d) | (me_t != t))(functools.partial(act, d, t))
                    else:
                        act(d, t)
            else:

                def step(index, carry):
                    d, t = lax.rem(index, n_dp), lax.div(index, n_dp)
                    wanted = group(d, t)
                    if skip:
                        wanted &= index != me_t * n_dp + me_d
                    pl.when(wanted)(functools.partial(act, d, t))
                    return carry

                lax.fori_loop(0, devices, step, 0)

        def line(count, mine, wanted, act):
            def step(index):
                pl.when((mine != index) & wanted(index))(functools.partial(act, index))

            repeat(count, step)

        half = n_t // 2
        my_half = me_t // half
        group = max(1, 8 // rows)
        blocks = half // group

        def gather_rows(which, index):
            d, start = index // blocks, which * half + index % blocks * group
            source = d * n_t + start
            block = jnp.concatenate(
                [normed_recv[source + k].astype(jnp.float32) for k in range(group)], axis=0
            )
            start = source * rows
            if not isinstance(start, int):
                start = pl.multiple_of(start, group * rows)
            normed_all[pl.ds(start, group * rows), :] = block

        fetch((gkv_hbm, gkv), (kv_up_hbm, kv_up), (gq_hbm, gq), (q_up_hbm, q_up))

        barrier = pltpu.get_barrier_semaphore()

        def greet(d, t):
            pl.semaphore_signal(barrier, inc=1, device_id=(d, t), device_id_type=mesh)

        pl.when(am_near)(functools.partial(each, near, True, greet))
        each(remote, True, greet)

        def send(source, target, kind, arrival, d, t):
            pltpu.make_async_remote_copy(
                src_ref=source,
                dst_ref=target,
                send_sem=send_sem.at[kind],
                recv_sem=recv_sem.at[arrival],
                device_id=(d, t),
                device_id_type=mesh,
            ).start()

        def send_sums(t):
            send(g_send.at[t], g_recv.at[me_t], 0, 0, me_d, t)

        def send_grads(d):
            send(grads, grads, 1, 1, d, me_t)

        def send_normed(d, t):
            send(normed_send.at[d], normed_recv.at[me], 2, 2 + my_half, d, t)

        def permit(d, t):
            pl.semaphore_signal(permit_sem, inc=1, device_id=(d, t), device_id_type=mesh)

        def sums_to(group):
            line(n_t, me_t, lambda t: group(me_d, t), send_sums)

        def grads_to(group):
            line(n_dp, me_d, lambda d: group(d, me_t), send_grads)

        @pl.when(am_first)
        def _():
            pl.semaphore_wait(barrier, nears - 1)

        @pl.when(am_last)
        def _():
            pl.semaphore_wait(barrier, devices - 1)
            each(near, False, permit)

        for load in loads[:4]:
            load.wait()
        unit_q[...], inverse = unit_rows(lq[...])
        inverse_q[...] = jnp.broadcast_to(inverse, inverse_q.shape)
        unit_kv[...], inverse = unit_rows(lkv[...])
        inverse_kv[...] = jnp.broadcast_to(inverse, inverse_kv.shape)
        normed_q = gain_q[...] * unit_q[...]
        normed_kv = gain_kv[...] * unit_kv[...]
        for d in range(n_dp):
            piece = jnp.concatenate(
                (
                    normed_q[:, d * q_part : (d + 1) * q_part],
                    normed_kv[:, d * kv_part : (d + 1) * kv_part],
                ),
                axis=1,
            )
            normed_send[d] = piece.astype(jnp.bfloat16)

        @pl.when(am_last)
        def _():
            each(near, False, send_normed)

        normed_recv[me] = normed_send[me_d]
        nt = (((1,), (1,)), ((), ()))

        def partial_sums(needed, cotangent, weights, start):
            for load in needed:
                load.wait()
            sums = lax.dot_general(
                cotangent[...], weights[...], nt, preferred_element_type=jnp.float32
            )
            span = slice(start, start + sums.shape[1])
            for t in range(n_t):
                g_send[t, :, span] = sums[t * rows : (t + 1) * rows].astype(g_send.dtype)

        partial_sums(loads[4:6], gkv, kv_up, q_width)

        @pl.when(am_remote & jnp.logical_not(am_last))
        def _():
            pl.semaphore_wait(barrier, devices - 1)
            each(first, False, send_normed)
            each(near, False, permit)

        partial_sums(loads[6:], gq, q_up, 0)
        g_recv[me_t] = g_send[me_t]

        @pl.when(am_near)
        def _():
            pl.when(jnp.logical_not(am_first))(lambda: pl.semaphore_wait(barrier, nears - 1))
            each(first, True, send_normed)
            sums_to(first)
            each(middle, True, send_normed)
            sums_to(middle)
            grads_to(near)
            pl.semaphore_wait(permit_sem, remotes)
            each(remote, False, send_normed)
            sums_to(remote)
            grads_to(remote)

        @pl.when(am_remote)
        def _():
            sums_to(first)

            @pl.when(jnp.logical_not(am_last))
            def _():
                each(middle, False, send_normed)

            sums_to(middle)
            each(remote, True, send_normed)
            sums_to(remote)
            grads_to(near)
            grads_to(remote)

        wait_bytes(all_grads.at[pl.ds(0, n_dp - 1)], recv_sem.at[1])
        for which in range(2):
            count = n_dp * half

            @pl.when(my_half == which)
            def _():
                wait_bytes(normed_recv.at[pl.ds(0, count - 1)], recv_sem.at[2 + which])

            @pl.when(my_half != which)
            def _():
                wait_bytes(normed_recv.at[pl.ds(0, count)], recv_sem.at[2 + which])

            repeat(n_dp * blocks, functools.partial(gather_rows, which))

        weight_gradient(d_q, normed_all, all_grads, slice(0, q_part), slice(0, q_cols))
        weight_gradient(d_kv, normed_all, all_grads, slice(q_part, None), slice(q_cols, None))
        wait_bytes(g_recv.at[pl.ds(0, n_t - 1)], send_sem.at[0])
        wait_bytes(all_grads.at[pl.ds(0, n_dp - 1)], send_sem.at[1])
        wait_bytes(normed_recv.at[pl.ds(0, devices - 1)], send_sem.at[2])
        wait_bytes(g_recv.at[pl.ds(0, n_t - 1)], recv_sem.at[0])

    pl.run_scoped(
        talk,
        pltpu.SemaphoreType.DMA((8,)),
        pltpu.SemaphoreType.DMA((3,)),
        pltpu.SemaphoreType.DMA((4,)),
        pltpu.SemaphoreType.REGULAR,
    )


def finish(
    g, all_grads, normed_all, unit_q, unit_kv, inverse_q, inverse_kv, gain_q, gain_kv, d_q, d_kv,
    out_q_hbm, out_kv_hbm, d_q_hbm, d_kv_hbm,
    out_q, out_kv,
    store_sem,
):
    stores = []

    def store(source, target):
        stores.append(pltpu.make_async_copy(source, target, store_sem.at[len(stores)]))
        stores[-1].start()

    store(d_q, d_q_hbm)
    n_t = g.shape[0]
    q_width = unit_q.shape[1]
    store(d_kv, d_kv_hbm)
    total = g[0].astype(jnp.float32)
    for t in range(1, n_t):
        total += g[t].astype(jnp.float32)
    out_q[...] = backward_of_norm(total[:, :q_width], unit_q[...], inverse_q[...], gain_q[...])
    out_kv[...] = backward_of_norm(total[:, q_width:], unit_kv[...], inverse_kv[...], gain_kv[...])
    store(out_q, out_q_hbm)
    store(out_kv, out_kv_hbm)
    for copy in stores:
        copy.wait()


def solution(mesh):
    n_dp, n_t = mesh.shape["dp"], mesh.shape["tensor"]

    def body(latent_q, latent_kv, gain_q, gain_kv, q_up, kv_up, grad_q, grad_kv):
        rows, q_width = latent_q.shape
        kv_width = latent_kv.shape[1]
        q_part, kv_part = q_width // n_dp, kv_width // n_dp
        part = q_part + kv_part
        width = q_width + kv_width
        devices = n_dp * n_t
        f32, bf16 = jnp.float32, jnp.bfloat16
        operands = (latent_q, latent_kv, gain_q, gain_kv, q_up, kv_up, grad_q, grad_kv)
        operands = [pltpu.with_memory_space_constraint(x, pltpu.HBM) for x in operands]
        hbm = pl.BlockSpec(memory_space=pltpu.HBM)

        vmem = pl.BlockSpec(memory_space=pltpu.VMEM)

        def like(x):
            return pltpu.VMEM(x.shape, x.dtype)

        results = (
            jax.ShapeDtypeStruct((rows, q_width), f32),
            jax.ShapeDtypeStruct((rows, kv_width), f32),
            jax.ShapeDtypeStruct((q_part, grad_q.shape[1]), f32),
            jax.ShapeDtypeStruct((kv_part, grad_kv.shape[1]), f32),
        )
        passed = (
            pltpu.VMEM((n_t, rows, width), bf16),
            pltpu.VMEM((n_dp, grad_q.shape[0], grad_q.shape[1] + grad_kv.shape[1]), bf16),
            pltpu.VMEM((devices * rows, part), f32),
            *(like(x) for x in results[:2] * 2),
            like(gain_q),
            like(gain_kv),
            like(results[2]),
            like(results[3]),
        )
        arrived = pl.pallas_call(
            functools.partial(exchange, n_dp, n_t),
            out_shape=passed,
            in_specs=[hbm] * len(operands),
            out_specs=(vmem,) * len(passed),
            scratch_shapes=[
                like(latent_q),
                like(latent_kv),
                pltpu.VMEM((devices, rows, part), bf16),
                *(like(x) for x in operands[4:6]),
                pltpu.VMEM((n_dp, rows, part), bf16),
                like(passed[0]),
            ],
            compiler_params=pltpu.CompilerParams(
                collective_id=0, has_side_effects=True, vmem_limit_bytes=LIMIT
            ),
        )(*operands)
        arrived = [pltpu.with_memory_space_constraint(x, pltpu.VMEM) for x in arrived]
        return pl.pallas_call(
            finish,
            out_shape=results,
            in_specs=[vmem] * len(arrived),
            out_specs=(hbm,) * 4,
            scratch_shapes=[
                *(like(x) for x in results[:2]),
                pltpu.SemaphoreType.DMA((4,)),
            ],
            compiler_params=pltpu.CompilerParams(vmem_limit_bytes=LIMIT),
        )(*arrived)

    return jax.shard_map(
        body,
        mesh=mesh,
        in_specs=(
            P(("dp", "tensor"), None),
            P(("dp", "tensor"), None),
            P(),
            P(),
            P(None, "tensor"),
            P(None, "tensor"),
            P("dp", "tensor"),
            P("dp", "tensor"),
        ),
        out_specs=(
            P(("dp", "tensor"), None),
            P(("dp", "tensor"), None),
            P("dp", "tensor"),
            P("dp", "tensor"),
        ),
        check_vma=False,
    )
```

```python
import functools

import jax
import jax.numpy as jnp
from jax import lax
from jax.experimental import pallas as pl
from jax.experimental.pallas import tpu as pltpu
from jax.sharding import PartitionSpec as P

EPS = 1e-06
UNROLL = 64
LIMIT = 24 * 1024 * 1024


def repeat(count, step):
    if count <= UNROLL:
        for index in range(count):
            step(index)
    else:

        def body(index, carry):
            step(index)
            return carry

        lax.fori_loop(0, count, body, 0)


def unit_rows(raw):
    values = raw.astype(jnp.float32)
    inverse = lax.rsqrt(jnp.mean(values * values, axis=-1, keepdims=True) + EPS)
    return values * inverse, inverse


def backward_of_norm(incoming, unit, inverse, gain):
    scaled = gain * incoming
    return inverse * (scaled - unit * jnp.mean(scaled * unit, axis=-1, keepdims=True))


def weight_gradient(target, normed_all, all_grads, rows, columns):
    tokens = normed_all.shape[0]
    target[...] = lax.dot_general(
        normed_all[:, rows].astype(jnp.bfloat16),
        all_grads[:, :, columns].reshape(tokens, -1),
        (((0,), (0,)), ((), ())),
        preferred_element_type=jnp.float32,
    )


def wait_bytes(ref, sem):
    pltpu.make_async_copy(ref, ref, sem).wait()


def exchange(
    n_dp, n_t,
    lq_hbm, lkv_hbm, gain_q_hbm, gain_kv_hbm, q_up_hbm, kv_up_hbm, gq_hbm, gkv_hbm,
    g_recv, all_grads, normed_all, unit_q, unit_kv, inverse_q, inverse_kv, gain_q, gain_kv, d_q, d_kv,
    lq, lkv, normed_recv, q_up, kv_up, normed_send, g_send,
):
    def talk(load_sem, send_sem, recv_sem, permit_sem):
        loads = []

        def fetch(*pairs):
            for source, target in pairs:
                loads.append(pltpu.make_async_copy(source, target, load_sem.at[len(loads)]))
                loads[-1].start()

        fetch((lq_hbm, lq), (lkv_hbm, lkv), (gain_q_hbm, gain_q), (gain_kv_hbm, gain_kv))
        me_d, me_t = lax.axis_index("dp"), lax.axis_index("tensor")
        me = me_d * n_t + me_t
        devices = n_dp * n_t
        rows = lq.shape[0]
        q_width, kv_width = lq.shape[1], lkv.shape[1]
        q_part, kv_part = q_width // n_dp, kv_width // n_dp
        q_cols = q_up.shape[1]
        grads = all_grads.at[me_d]
        gq, gkv = grads.at[:, :q_cols], grads.at[:, q_cols:]
        mesh = pl.DeviceIdType.MESH

        def depth(d, t):
            return t // 2 + t % 2 + d // 2

        everyone = [(d, t) for d in range(n_dp) for t in range(n_t)]
        everyone.sort(key=lambda place: depth(*place))
        deepest = depth(*everyone[-1])

        def remote(d, t):
            return depth(d, t) >= max(1, deepest - 1)

        def near(d, t):
            return depth(d, t) < max(1, deepest - 1)

        def first(d, t):
            return (t == 0) & (d < 2)

        def middle(d, t):
            return near(d, t) & ((t != 0) | (d >= 2))

        remotes = sum(int(remote(d, t)) for d, t in everyone)
        nears = devices - remotes
        am_first = first(me_d, me_t)
        am_near = near(me_d, me_t)
        am_remote = remote(me_d, me_t)
        am_last = depth(me_d, me_t) == deepest

        def each(group, skip, act):
            if devices <= UNROLL:
                for d, t in everyone:
                    if not group(d, t):
                        continue
                    if skip:
                        pl.when((me_d != d) | (me_t != t))(functools.partial(act, d, t))
                    else:
                        act(d, t)
            else:

                def step(index, carry):
                    d, t = lax.rem(index, n_dp), lax.div(index, n_dp)
                    wanted = group(d, t)
                    if skip:
                        wanted &= index != me_t * n_dp + me_d
                    pl.when(wanted)(functools.partial(act, d, t))
                    return carry

                lax.fori_loop(0, devices, step, 0)

        def line(count, mine, wanted, act):
            def step(index):
                pl.when((mine != index) & wanted(index))(functools.partial(act, index))

            repeat(count, step)

        half = n_t // 2
        my_half = me_t // half
        group = max(1, 8 // rows)
        blocks = half // group

        def gather_rows(which, index):
            d, start = index // blocks, which * half + index % blocks * group
            source = d * n_t + start
            block = jnp.concatenate(
                [normed_recv[source + k].astype(jnp.float32) for k in range(group)], axis=0
            )
            start = source * rows
            if not isinstance(start, int):
                start = pl.multiple_of(start, group * rows)
            normed_all[pl.ds(start, group * rows), :] = block

        fetch((gkv_hbm, gkv), (kv_up_hbm, kv_up), (gq_hbm, gq), (q_up_hbm, q_up))

        barrier = pltpu.get_barrier_semaphore()

        def greet(d, t):
            pl.semaphore_signal(barrier, inc=1, device_id=(d, t), device_id_type=mesh)

        pl.when(am_near)(functools.partial(each, near, True, greet))
        each(remote, True, greet)

        def send(source, target, kind, arrival, d, t):
            pltpu.make_async_remote_copy(
                src_ref=source,
                dst_ref=target,
                send_sem=send_sem.at[kind],
                recv_sem=recv_sem.at[arrival],
                device_id=(d, t),
                device_id_type=mesh,
            ).start()

        def send_sums(t):
            send(g_send.at[t], g_recv.at[me_t], 0, 0, me_d, t)

        def send_grads(d):
            send(grads, grads, 1, 1, d, me_t)

        def send_normed(d, t):
            send(normed_send.at[d], normed_recv.at[me], 2, 2 + my_half, d, t)

        def permit(d, t):
            pl.semaphore_signal(permit_sem, inc=1, device_id=(d, t), device_id_type=mesh)

        def sums_to(group):
            line(n_t, me_t, lambda t: group(me_d, t), send_sums)

        def grads_to(group):
            line(n_dp, me_d, lambda d: group(d, me_t), send_grads)

        @pl.when(am_first)
        def _():
            pl.semaphore_wait(barrier, nears - 1)

        @pl.when(am_last)
        def _():
            pl.semaphore_wait(barrier, devices - 1)
            each(near, False, permit)

        for load in loads[:4]:
            load.wait()
        unit_q[...], inverse = unit_rows(lq[...])
        inverse_q[...] = jnp.broadcast_to(inverse, inverse_q.shape)
        unit_kv[...], inverse = unit_rows(lkv[...])
        inverse_kv[...] = jnp.broadcast_to(inverse, inverse_kv.shape)
        normed_q = gain_q[...] * unit_q[...]
        normed_kv = gain_kv[...] * unit_kv[...]
        for d in range(n_dp):
            piece = jnp.concatenate(
                (
                    normed_q[:, d * q_part : (d + 1) * q_part],
                    normed_kv[:, d * kv_part : (d + 1) * kv_part],
                ),
                axis=1,
            )
            normed_send[d] = piece.astype(jnp.bfloat16)

        @pl.when(am_last)
        def _():
            each(near, False, send_normed)

        normed_recv[me] = normed_send[me_d]
        nt = (((1,), (1,)), ((), ()))

        def partial_sums(needed, cotangent, weights, start):
            for load in needed:
                load.wait()
            sums = lax.dot_general(
                cotangent[...], weights[...], nt, preferred_element_type=jnp.float32
            )
            span = slice(start, start + sums.shape[1])
            for t in range(n_t):
                g_send[t, :, span] = sums[t * rows : (t + 1) * rows].astype(g_send.dtype)

        partial_sums(loads[4:6], gkv, kv_up, q_width)

        @pl.when(am_remote & jnp.logical_not(am_last))
        def _():
            pl.semaphore_wait(barrier, devices - 1)
            each(first, False, send_normed)
            each(near, False, permit)

        partial_sums(loads[6:], gq, q_up, 0)
        g_recv[me_t] = g_send[me_t]

        @pl.when(am_near)
        def _():
            pl.when(jnp.logical_not(am_first))(lambda: pl.semaphore_wait(barrier, nears - 1))
            each(first, True, send_normed)
            sums_to(first)
            each(middle, True, send_normed)
            sums_to(middle)
            grads_to(near)
            pl.semaphore_wait(permit_sem, remotes)
            each(remote, False, send_normed)
            sums_to(remote)
            grads_to(remote)

        @pl.when(am_remote)
        def _():
            sums_to(first)

            @pl.when(jnp.logical_not(am_last))
            def _():
                each(middle, False, send_normed)

            sums_to(middle)
            each(remote, True, send_normed)
            sums_to(remote)
            grads_to(near)
            grads_to(remote)

        wait_bytes(all_grads.at[pl.ds(0, n_dp - 1)], recv_sem.at[1])
        for which in range(2):
            count = n_dp * half

            @pl.when(my_half == which)
            def _():
                wait_bytes(normed_recv.at[pl.ds(0, count - 1)], recv_sem.at[2 + which])

            @pl.when(my_half != which)
            def _():
                wait_bytes(normed_recv.at[pl.ds(0, count)], recv_sem.at[2 + which])

            repeat(n_dp * blocks, functools.partial(gather_rows, which))

        weight_gradient(d_q, normed_all, all_grads, slice(0, q_part), slice(0, q_cols))
        weight_gradient(d_kv, normed_all, all_grads, slice(q_part, None), slice(q_cols, None))
        wait_bytes(g_recv.at[pl.ds(0, n_t - 1)], send_sem.at[0])
        wait_bytes(all_grads.at[pl.ds(0, n_dp - 1)], send_sem.at[1])
        wait_bytes(normed_recv.at[pl.ds(0, devices - 1)], send_sem.at[2])
        wait_bytes(g_recv.at[pl.ds(0, n_t - 1)], recv_sem.at[0])

    pl.run_scoped(
        talk,
        pltpu.SemaphoreType.DMA((8,)),
        pltpu.SemaphoreType.DMA((3,)),
        pltpu.SemaphoreType.DMA((4,)),
        pltpu.SemaphoreType.REGULAR,
    )


def finish(
    g, all_grads, normed_all, unit_q, unit_kv, inverse_q, inverse_kv, gain_q, gain_kv, d_q, d_kv,
    out_q_hbm, out_kv_hbm, d_q_hbm, d_kv_hbm,
    out_q, out_kv,
):
    def work(store_sem):
        stores = []

        def store(source, target):
            stores.append(pltpu.make_async_copy(source, target, store_sem.at[len(stores)]))
            stores[-1].start()

        store(d_q, d_q_hbm)
        n_t = g.shape[0]
        q_width = unit_q.shape[1]
        store(d_kv, d_kv_hbm)
        total = g[0].astype(jnp.float32)
        for t in range(1, n_t):
            total += g[t].astype(jnp.float32)
        out_q[...] = backward_of_norm(total[:, :q_width], unit_q[...], inverse_q[...], gain_q[...])
        out_kv[...] = backward_of_norm(total[:, q_width:], unit_kv[...], inverse_kv[...], gain_kv[...])
        store(out_q, out_q_hbm)
        store(out_kv, out_kv_hbm)
        for copy in stores:
            copy.wait()

    pl.run_scoped(work, pltpu.SemaphoreType.DMA((4,)))


def solution(mesh):
    n_dp, n_t = mesh.shape["dp"], mesh.shape["tensor"]

    def body(latent_q, latent_kv, gain_q, gain_kv, q_up, kv_up, grad_q, grad_kv):
        rows, q_width = latent_q.shape
        kv_width = latent_kv.shape[1]
        q_part, kv_part = q_width // n_dp, kv_width // n_dp
        part = q_part + kv_part
        width = q_width + kv_width
        devices = n_dp * n_t
        f32, bf16 = jnp.float32, jnp.bfloat16
        operands = (latent_q, latent_kv, gain_q, gain_kv, q_up, kv_up, grad_q, grad_kv)
        operands = [pltpu.with_memory_space_constraint(x, pltpu.HBM) for x in operands]
        hbm = pl.BlockSpec(memory_space=pltpu.HBM)

        vmem = pl.BlockSpec(memory_space=pltpu.VMEM)

        def like(x):
            return pltpu.VMEM(x.shape, x.dtype)

        results = (
            jax.ShapeDtypeStruct((rows, q_width), f32),
            jax.ShapeDtypeStruct((rows, kv_width), f32),
            jax.ShapeDtypeStruct((q_part, grad_q.shape[1]), f32),
            jax.ShapeDtypeStruct((kv_part, grad_kv.shape[1]), f32),
        )
        passed = (
            pltpu.VMEM((n_t, rows, width), bf16),
            pltpu.VMEM((n_dp, grad_q.shape[0], grad_q.shape[1] + grad_kv.shape[1]), bf16),
            pltpu.VMEM((devices * rows, part), f32),
            *(like(x) for x in results[:2] * 2),
            like(gain_q),
            like(gain_kv),
            like(results[2]),
            like(results[3]),
        )
        arrived = pl.pallas_call(
            functools.partial(exchange, n_dp, n_t),
            out_shape=passed,
            in_specs=[hbm] * len(operands),
            out_specs=(vmem,) * len(passed),
            scratch_shapes=[
                like(latent_q),
                like(latent_kv),
                pltpu.VMEM((devices, rows, part), bf16),
                *(like(x) for x in operands[4:6]),
                pltpu.VMEM((n_dp, rows, part), bf16),
                like(passed[0]),
            ],
            compiler_params=pltpu.CompilerParams(
                collective_id=0, has_side_effects=True, vmem_limit_bytes=LIMIT
            ),
        )(*operands)
        arrived = [pltpu.with_memory_space_constraint(x, pltpu.VMEM) for x in arrived]
        return pl.pallas_call(
            finish,
            out_shape=results,
            in_specs=[vmem] * len(arrived),
            out_specs=(hbm,) * 4,
            scratch_shapes=[
                *(like(x) for x in results[:2]),
            ],
            compiler_params=pltpu.CompilerParams(vmem_limit_bytes=LIMIT),
        )(*arrived)

    return jax.shard_map(
        body,
        mesh=mesh,
        in_specs=(
            P(("dp", "tensor"), None),
            P(("dp", "tensor"), None),
            P(),
            P(),
            P(None, "tensor"),
            P(None, "tensor"),
            P("dp", "tensor"),
            P("dp", "tensor"),
        ),
        out_specs=(
            P(("dp", "tensor"), None),
            P(("dp", "tensor"), None),
            P("dp", "tensor"),
            P("dp", "tensor"),
        ),
        check_vma=False,
    )
```

```python
import functools

import jax
import jax.numpy as jnp
from jax import lax
from jax.experimental import pallas as pl
from jax.experimental.pallas import tpu as pltpu
from jax.sharding import PartitionSpec as P

EPS = 1e-06
UNROLL = 64
PARTS = 4
LIMIT = 24 * 1024 * 1024


def repeat(count, step):
    if count <= UNROLL:
        for index in range(count):
            step(index)
    else:

        def body(index, carry):
            step(index)
            return carry

        lax.fori_loop(0, count, body, 0)


def unit_rows(raw):
    values = raw.astype(jnp.float32)
    inverse = lax.rsqrt(jnp.mean(values * values, axis=-1, keepdims=True) + EPS)
    return values * inverse, inverse


def backward_of_norm(incoming, unit, inverse, gain):
    scaled = gain * incoming
    return inverse * (scaled - unit * jnp.mean(scaled * unit, axis=-1, keepdims=True))


def weight_gradient(target, normed_all, all_grads, rows, columns):
    tokens = normed_all.shape[0]
    target[...] = lax.dot_general(
        normed_all[:, rows].astype(jnp.bfloat16),
        all_grads[:, :, columns].reshape(tokens, -1),
        (((0,), (0,)), ((), ())),
        preferred_element_type=jnp.float32,
    )


def wait_bytes(ref, sem):
    pltpu.make_async_copy(ref, ref, sem).wait()


def exchange(
    n_dp, n_t,
    lq_hbm, lkv_hbm, gain_q_hbm, gain_kv_hbm, q_up_hbm, kv_up_hbm, gq_hbm, gkv_hbm,
    g_recv, all_grads, normed_all, unit_q, unit_kv, inverse_q, inverse_kv, gain_q, gain_kv, d_q, d_kv,
    lq, lkv, normed_recv, q_up, kv_up, normed_send, g_send,
):
    def talk(load_sem, send_sem, recv_sem, permit_sem):
        loads = []

        def fetch(*pairs):
            for source, target in pairs:
                loads.append(pltpu.make_async_copy(source, target, load_sem.at[len(loads)]))
                loads[-1].start()

        fetch((lq_hbm, lq), (lkv_hbm, lkv), (gain_q_hbm, gain_q), (gain_kv_hbm, gain_kv))
        me_d, me_t = lax.axis_index("dp"), lax.axis_index("tensor")
        me = me_d * n_t + me_t
        devices = n_dp * n_t
        rows = lq.shape[0]
        q_width, kv_width = lq.shape[1], lkv.shape[1]
        q_part, kv_part = q_width // n_dp, kv_width // n_dp
        q_cols = q_up.shape[1]
        grads = all_grads.at[me_d]
        gq, gkv = grads.at[:, :q_cols], grads.at[:, q_cols:]
        mesh = pl.DeviceIdType.MESH

        def depth(d, t):
            return t // 2 + t % 2 + d // 2

        everyone = [(d, t) for d in range(n_dp) for t in range(n_t)]
        everyone.sort(key=lambda place: depth(*place))
        deepest = depth(*everyone[-1])

        def remote(d, t):
            return depth(d, t) >= max(1, deepest - 1)

        def near(d, t):
            return depth(d, t) < max(1, deepest - 1)

        def first(d, t):
            return (t == 0) & (d < 2)

        def middle(d, t):
            return near(d, t) & ((t != 0) | (d >= 2))

        remotes = sum(int(remote(d, t)) for d, t in everyone)
        nears = devices - remotes
        am_first = first(me_d, me_t)
        am_near = near(me_d, me_t)
        am_remote = remote(me_d, me_t)
        am_last = depth(me_d, me_t) == deepest

        def each(group, skip, act):
            if devices <= UNROLL:
                for d, t in everyone:
                    if not group(d, t):
                        continue
                    if skip:
                        pl.when((me_d != d) | (me_t != t))(functools.partial(act, d, t))
                    else:
                        act(d, t)
            else:

                def step(index, carry):
                    d, t = lax.rem(index, n_dp), lax.div(index, n_dp)
                    wanted = group(d, t)
                    if skip:
                        wanted &= index != me_t * n_dp + me_d
                    pl.when(wanted)(functools.partial(act, d, t))
                    return carry

                lax.fori_loop(0, devices, step, 0)

        def line(count, mine, wanted, act):
            def step(index):
                pl.when((mine != index) & wanted(index))(functools.partial(act, index))

            repeat(count, step)

        half = n_t // PARTS
        my_half = me_t // half
        group = min(max(1, 8 // rows), half)
        blocks = half // group

        def gather_rows(which, index):
            d, start = index // blocks, which * half + index % blocks * group
            source = d * n_t + start
            block = jnp.concatenate(
                [normed_recv[source + k].astype(jnp.float32) for k in range(group)], axis=0
            )
            start = source * rows
            if not isinstance(start, int):
                start = pl.multiple_of(start, group * rows)
            normed_all[pl.ds(start, group * rows), :] = block

        fetch((gkv_hbm, gkv), (kv_up_hbm, kv_up), (gq_hbm, gq), (q_up_hbm, q_up))

        barrier = pltpu.get_barrier_semaphore()

        def greet(d, t):
            pl.semaphore_signal(barrier, inc=1, device_id=(d, t), device_id_type=mesh)

        pl.when(am_near)(functools.partial(each, near, True, greet))
        each(remote, True, greet)

        def send(source, target, kind, arrival, d, t):
            pltpu.make_async_remote_copy(
                src_ref=source,
                dst_ref=target,
                send_sem=send_sem.at[kind],
                recv_sem=recv_sem.at[arrival],
                device_id=(d, t),
                device_id_type=mesh,
            ).start()

        def send_sums(t):
            send(g_send.at[t], g_recv.at[me_t], 0, 0, me_d, t)

        def send_grads(d):
            send(grads, grads, 1, 1, d, me_t)

        def send_normed(d, t):
            send(normed_send.at[d], normed_recv.at[me], 2, 2 + my_half, d, t)

        def permit(d, t):
            pl.semaphore_signal(permit_sem, inc=1, device_id=(d, t), device_id_type=mesh)

        def sums_to(group):
            line(n_t, me_t, lambda t: group(me_d, t), send_sums)

        def grads_to(group):
            line(n_dp, me_d, lambda d: group(d, me_t), send_grads)

        @pl.when(am_first)
        def _():
            pl.semaphore_wait(barrier, nears - 1)

        @pl.when(am_last)
        def _():
            pl.semaphore_wait(barrier, devices - 1)
            each(near, False, permit)

        for load in loads[:4]:
            load.wait()
        unit_q[...], inverse = unit_rows(lq[...])
        inverse_q[...] = jnp.broadcast_to(inverse, inverse_q.shape)
        unit_kv[...], inverse = unit_rows(lkv[...])
        inverse_kv[...] = jnp.broadcast_to(inverse, inverse_kv.shape)
        normed_q = gain_q[...] * unit_q[...]
        normed_kv = gain_kv[...] * unit_kv[...]
        for d in range(n_dp):
            piece = jnp.concatenate(
                (
                    normed_q[:, d * q_part : (d + 1) * q_part],
                    normed_kv[:, d * kv_part : (d + 1) * kv_part],
                ),
                axis=1,
            )
            normed_send[d] = piece.astype(jnp.bfloat16)

        @pl.when(am_last)
        def _():
            each(near, False, send_normed)

        normed_recv[me] = normed_send[me_d]
        nt = (((1,), (1,)), ((), ()))

        def partial_sums(needed, cotangent, weights, start):
            for load in needed:
                load.wait()
            sums = lax.dot_general(
                cotangent[...], weights[...], nt, preferred_element_type=jnp.float32
            )
            span = slice(start, start + sums.shape[1])
            for t in range(n_t):
                g_send[t, :, span] = sums[t * rows : (t + 1) * rows].astype(g_send.dtype)

        partial_sums(loads[4:6], gkv, kv_up, q_width)

        @pl.when(am_remote & jnp.logical_not(am_last))
        def _():
            pl.semaphore_wait(barrier, devices - 1)
            each(first, False, send_normed)
            each(near, False, permit)

        partial_sums(loads[6:], gq, q_up, 0)
        g_recv[me_t] = g_send[me_t]

        @pl.when(am_near)
        def _():
            pl.when(jnp.logical_not(am_first))(lambda: pl.semaphore_wait(barrier, nears - 1))
            each(first, True, send_normed)
            sums_to(first)
            each(middle, True, send_normed)
            sums_to(middle)
            grads_to(near)
            pl.semaphore_wait(permit_sem, remotes)
            each(remote, False, send_normed)
            sums_to(remote)
            grads_to(remote)

        @pl.when(am_remote)
        def _():
            sums_to(first)

            @pl.when(jnp.logical_not(am_last))
            def _():
                each(middle, False, send_normed)

            sums_to(middle)
            each(remote, True, send_normed)
            sums_to(remote)
            grads_to(near)
            grads_to(remote)

        wait_bytes(all_grads.at[pl.ds(0, n_dp - 1)], recv_sem.at[1])
        for which in range(PARTS):
            count = n_dp * half

            @pl.when(my_half == which)
            def _():
                wait_bytes(normed_recv.at[pl.ds(0, count - 1)], recv_sem.at[2 + which])

            @pl.when(my_half != which)
            def _():
                wait_bytes(normed_recv.at[pl.ds(0, count)], recv_sem.at[2 + which])

            repeat(n_dp * blocks, functools.partial(gather_rows, which))

        weight_gradient(d_q, normed_all, all_grads, slice(0, q_part), slice(0, q_cols))
        weight_gradient(d_kv, normed_all, all_grads, slice(q_part, None), slice(q_cols, None))
        wait_bytes(g_recv.at[pl.ds(0, n_t - 1)], send_sem.at[0])
        wait_bytes(all_grads.at[pl.ds(0, n_dp - 1)], send_sem.at[1])
        wait_bytes(normed_recv.at[pl.ds(0, devices - 1)], send_sem.at[2])
        wait_bytes(g_recv.at[pl.ds(0, n_t - 1)], recv_sem.at[0])

    pl.run_scoped(
        talk,
        pltpu.SemaphoreType.DMA((8,)),
        pltpu.SemaphoreType.DMA((3,)),
        pltpu.SemaphoreType.DMA((2 + PARTS,)),
        pltpu.SemaphoreType.REGULAR,
    )


def finish(
    g, all_grads, normed_all, unit_q, unit_kv, inverse_q, inverse_kv, gain_q, gain_kv, d_q, d_kv,
    out_q_hbm, out_kv_hbm, d_q_hbm, d_kv_hbm,
    out_q, out_kv,
):
    def work(store_sem):
        stores = []

        def store(source, target):
            stores.append(pltpu.make_async_copy(source, target, store_sem.at[len(stores)]))
            stores[-1].start()

        store(d_q, d_q_hbm)
        n_t = g.shape[0]
        q_width = unit_q.shape[1]
        store(d_kv, d_kv_hbm)
        total = g[0].astype(jnp.float32)
        for t in range(1, n_t):
            total += g[t].astype(jnp.float32)
        out_q[...] = backward_of_norm(total[:, :q_width], unit_q[...], inverse_q[...], gain_q[...])
        out_kv[...] = backward_of_norm(total[:, q_width:], unit_kv[...], inverse_kv[...], gain_kv[...])
        store(out_q, out_q_hbm)
        store(out_kv, out_kv_hbm)
        for copy in stores:
            copy.wait()

    pl.run_scoped(work, pltpu.SemaphoreType.DMA((4,)))


def solution(mesh):
    n_dp, n_t = mesh.shape["dp"], mesh.shape["tensor"]

    def body(latent_q, latent_kv, gain_q, gain_kv, q_up, kv_up, grad_q, grad_kv):
        rows, q_width = latent_q.shape
        kv_width = latent_kv.shape[1]
        q_part, kv_part = q_width // n_dp, kv_width // n_dp
        part = q_part + kv_part
        width = q_width + kv_width
        devices = n_dp * n_t
        f32, bf16 = jnp.float32, jnp.bfloat16
        operands = (latent_q, latent_kv, gain_q, gain_kv, q_up, kv_up, grad_q, grad_kv)
        operands = [pltpu.with_memory_space_constraint(x, pltpu.HBM) for x in operands]
        hbm = pl.BlockSpec(memory_space=pltpu.HBM)

        vmem = pl.BlockSpec(memory_space=pltpu.VMEM)

        def like(x):
            return pltpu.VMEM(x.shape, x.dtype)

        results = (
            jax.ShapeDtypeStruct((rows, q_width), f32),
            jax.ShapeDtypeStruct((rows, kv_width), f32),
            jax.ShapeDtypeStruct((q_part, grad_q.shape[1]), f32),
            jax.ShapeDtypeStruct((kv_part, grad_kv.shape[1]), f32),
        )
        passed = (
            pltpu.VMEM((n_t, rows, width), bf16),
            pltpu.VMEM((n_dp, grad_q.shape[0], grad_q.shape[1] + grad_kv.shape[1]), bf16),
            pltpu.VMEM((devices * rows, part), f32),
            *(like(x) for x in results[:2] * 2),
            like(gain_q),
            like(gain_kv),
            like(results[2]),
            like(results[3]),
        )
        arrived = pl.pallas_call(
            functools.partial(exchange, n_dp, n_t),
            out_shape=passed,
            in_specs=[hbm] * len(operands),
            out_specs=(vmem,) * len(passed),
            scratch_shapes=[
                like(latent_q),
                like(latent_kv),
                pltpu.VMEM((devices, rows, part), bf16),
                *(like(x) for x in operands[4:6]),
                pltpu.VMEM((n_dp, rows, part), bf16),
                like(passed[0]),
            ],
            compiler_params=pltpu.CompilerParams(
                collective_id=0, has_side_effects=True, vmem_limit_bytes=LIMIT
            ),
        )(*operands)
        arrived = [pltpu.with_memory_space_constraint(x, pltpu.VMEM) for x in arrived]
        return pl.pallas_call(
            finish,
            out_shape=results,
            in_specs=[vmem] * len(arrived),
            out_specs=(hbm,) * 4,
            scratch_shapes=[
                *(like(x) for x in results[:2]),
            ],
            compiler_params=pltpu.CompilerParams(vmem_limit_bytes=LIMIT),
        )(*arrived)

    return jax.shard_map(
        body,
        mesh=mesh,
        in_specs=(
            P(("dp", "tensor"), None),
            P(("dp", "tensor"), None),
            P(),
            P(),
            P(None, "tensor"),
            P(None, "tensor"),
            P("dp", "tensor"),
            P("dp", "tensor"),
        ),
        out_specs=(
            P(("dp", "tensor"), None),
            P(("dp", "tensor"), None),
            P("dp", "tensor"),
            P("dp", "tensor"),
        ),
        check_vma=False,
    )
```
